256 devices in a mesh: grp: 2 (over z), tp: 128 (over x, y, core).
Axes of the slice: x: 8, y: 8, z: 2, core: 2. Of those that a mesh axis runs over, the one named last changes fastest.
The devices are a block of a 8x8x16 slice.
Arguments:
- hidden_in: float32 [64, 4608], P('grp'), parts along dimension 0, may hold values from -6 to 6
- prefill_cache: bfloat16 [128, 1, 2, 4, 128, 8, 256], P('tp', None, None, 'grp'), parts along dimension 3, may hold values from -6 to 6
- lengths: int32 [64], P('grp'), parts along dimension 0, may hold values from 1 to 1023
- page_table: int32 [64, 128], P('grp'), parts along dimension 0, may hold values from 0 to 127, each once within a row
- qkv_weight: bfloat16 [1, 8192, 4608], P(None, 'tp'), may hold values from -0.09375 to 0.09375
- out_weight: bfloat16 [1, 4608, 4096], P(None, 'tp'), may hold values from -0.09375 to 0.09375
- gate_up_weight: bfloat16 [1, 2, 18432, 4608], P(None, None, 'tp'), may hold values from -0.09375 to 0.09375
- down_weight: bfloat16 [1, 18432, 4608], P(None, 'tp'), may hold values from -0.15625 to 0.15625
- norm_gains: float32 [1, 4, 4608], replicated, may hold values from 0.25 to 1.75
Outputs:
- hidden_out: float32 [64, 4608], P('grp', 'tp'), parts along dimension 0
- decode_cache: bfloat16 [128, 1, 2, 64, 8, 2048], P('tp', None, None, 'grp'), parts along dimension 3
The draws below stay inside these ranges and needn't reach their ends.
There are 2 independent parts, one for each index of `grp`. The reference program is written for one: setup_inputs(seed, part) draws one part's arguments, and reference() takes and returns one part's arrays. A program takes and returns all parts, laid end to end along the dimension named above; an argument that names none is the same for every part. Nothing has to cross between parts.
Inputs may be any that keep to these rules, and one draw needn't show every extreme that they name: Request r's new token takes position lengths[r]. Each row is a permutation of 0 to 127; page j of request r holds cache positions page_table[r, j] * 8 to page_table[r, j] * 8 + 7.
All inputs are finite; a program needn't handle non-finite values.
Results may differ from the reference program's by a relative error of at most 0.012.
The reference program's roundings to bfloat16 on the way (of `normed`, `projected`, `attended`, `mixed`, `ffn_in` and `active`) count: a program that leaves them out, or rounds other values in their place, can miss the bound.
Values may be sent and summed in bfloat16 or wider, within the bound.
A program may use at most 64 MiB of HBM per device.

```python
import jax
import jax.numpy as jnp
from jax import lax

D = 4608
HEADS = 32
KV_HEADS = 16
HEAD_DIM = 128
FF = 18432
PREFILL_TP = 8
LAYERS = 1
REQ_GROUP = 2
CTX_DEV = 8
BATCH = 32
CTX = 1024
N_TP = 128


def touch_ends(entries, rng, smallest, high):
    spot = [jax.random.randint(jax.random.fold_in(rng, axis), (), 0, length) for axis, length in enumerate(entries.shape)]
    longest = entries.shape.index(max(entries.shape))
    next_to = spot[:longest] + [(spot[longest] + 1) % entries.shape[longest]] + spot[longest + 1:]
    return entries.at[tuple(spot)].set(smallest).at[tuple(next_to)].set(high)


def with_spikes(entries, own_key, source, target, blocks, factor):
    owner, partner = [(jnp.arange(entries.shape[axis_at]) // (entries.shape[axis_at] // blocks)).reshape([-1 if axis == axis_at else 1 for axis in range(entries.ndim)]) for axis_at in (source, target)]
    chosen = jax.random.permutation(own_key, blocks)[partner]
    strong = (owner == chosen) | (owner == (partner + blocks // 2) % blocks)
    return jnp.where(strong, factor * entries, entries)


def level_of(key, dims, pieces, smallest, largest):
    gain, own = 1.0, jax.random.fold_in(key, 6)
    for position, blocks in pieces:
        draws = jnp.exp(jax.random.uniform(jax.random.fold_in(own, position), (blocks,), jnp.float32, smallest / len(pieces), largest / len(pieces)))
        gain = gain * jnp.repeat(draws, dims[position] // blocks).reshape([-1 if axis == position else 1 for axis in range(len(dims))])
    return gain


def gaussian(stream_key, shape, width, most, cuts=(), kind=jnp.bfloat16):
    loudness = level_of(stream_key, shape, cuts, -0.22, 0.18) if cuts else 1.0
    drawn = jax.random.normal(stream_key, shape, jnp.float32) * width * loudness
    return jnp.minimum(jnp.maximum(drawn, -most), most).astype(kind)


def bell_draw_with(key, shape, deviation, reach, split, heavy, kind=jnp.bfloat16):
    array = deviation * jax.random.normal(key, shape, jnp.float32)
    if split:
        array = array * level_of(key, shape, split, -0.22, 0.18)
    return jnp.clip(with_spikes(array, jax.random.fold_in(key, 3), *heavy), -reach, reach).astype(kind)


def setup_inputs(seed: int = 0, part: int = 0) -> dict:
    key_list = jax.random.split(jax.random.key(seed), 10)
    own_keys = jax.random.split(jax.random.fold_in(key_list[9], part), 10)
    hidden_in = gaussian(own_keys[0], (BATCH, D), 1.0, 6.0, (), jnp.float32)
    prefill_cache = gaussian(own_keys[1], (N_TP, LAYERS, 2, REQ_GROUP, N_TP, CTX_DEV, KV_HEADS // PREFILL_TP * HEAD_DIM), 1.0, 6.0, ((0, 128),))
    lengths = touch_ends(jax.random.randint(own_keys[2], (BATCH,), 1, CTX), jax.random.fold_in(own_keys[2], 1), 1, CTX - 1).astype(jnp.int32)
    page_table = jax.vmap(lambda own: jax.random.permutation(own, N_TP))(jax.random.split(own_keys[3], BATCH)).reshape((BATCH, N_TP)).astype(jnp.int32)
    qkv_weight = gaussian(key_list[4], (LAYERS, (HEADS + 2 * KV_HEADS) * HEAD_DIM, D), D ** -0.5, 0.09375, ((1, 128),))
    out_weight = gaussian(key_list[5], (LAYERS, D, HEADS * HEAD_DIM), (HEADS * HEAD_DIM) ** -0.5, 0.09375, ((1, 128),))
    gate_up_weight = gaussian(key_list[6], (LAYERS, 2, FF, D), D ** -0.5, 0.09375, ((2, 128),))
    down_weight = bell_draw_with(key_list[7], (LAYERS, FF, D), FF ** -0.5, 0.15625, ((1, 128),), (1, 2, 128, 5.5))
    norm_gains = jnp.clip(1.0 + 0.15 * jax.random.normal(key_list[8], (LAYERS, 4, D), jnp.float32), 0.25, 1.75)
    return dict(hidden_in=hidden_in, prefill_cache=prefill_cache, lengths=lengths, page_table=page_table, qkv_weight=qkv_weight, out_weight=out_weight, gate_up_weight=gate_up_weight, down_weight=down_weight, norm_gains=norm_gains)


EPSILON = 1e-06
SOFTCAP = 50.0

def rms_scale(vector, gain_row):
    meansq = lax.optimization_barrier(jnp.mean(vector * vector, axis=-1, keepdims=True))
    return vector * lax.rsqrt(meansq + EPSILON) * (1.0 + gain_row)

def rotate(vector, positions):
    half_dim = vector.shape[-1] // 2
    exponent = jnp.arange(half_dim, dtype=jnp.float32) * (-2.0 / vector.shape[-1])
    frequency = jnp.power(jnp.float32(10000.0), exponent)
    angles = positions.astype(jnp.float32)[:, None, None] * frequency
    cosine = jnp.cos(angles)
    sine_term = jnp.sin(angles)
    front_half = vector[..., :half_dim]
    back_half = vector[..., half_dim:]
    return jnp.concatenate([front_half * cosine - back_half * sine_term, back_half * cosine + front_half * sine_term], axis=-1)

def capped(raw_scores):
    return SOFTCAP * jnp.tanh(raw_scores / SOFTCAP)

def round_back(vector):
    return lax.optimization_barrier(vector.astype(jnp.bfloat16)).astype(jnp.float32)

def reference(hidden_in, prefill_cache, lengths, page_table, qkv_weight, out_weight, gate_up_weight, down_weight, norm_gains):
    groups = N_TP // PREFILL_TP
    local_heads = KV_HEADS // PREFILL_TP
    head_share = HEADS // KV_HEADS
    score_scale = (D / HEADS) ** (-0.5)
    q_cols = HEADS * HEAD_DIM
    k_cols = KV_HEADS * HEAD_DIM
    blocks = prefill_cache.reshape(groups, PREFILL_TP, LAYERS, 2, REQ_GROUP, N_TP, CTX_DEV, local_heads, HEAD_DIM)
    by_request = blocks.transpose(2, 3, 0, 4, 5, 6, 1, 7, 8).reshape(LAYERS, 2, BATCH, N_TP, CTX_DEV, k_cols)
    page_ids = jnp.arange(N_TP, dtype=jnp.int32)
    onehot = (page_table[:, :, None] == page_ids[None, None, :]).astype(jnp.int32)
    inverse = lax.optimization_barrier(jnp.sum(onehot * page_ids[None, :, None], axis=1)).astype(jnp.int32)
    ordered = jnp.take_along_axis(by_request, inverse[None, None, :, :, None, None], axis=3)
    positions = page_ids[:, None] * CTX_DEV + jnp.arange(CTX_DEV, dtype=jnp.int32)[None, :]
    visible = positions[None, :, :] < lengths[:, None, None]
    fresh_slot = positions[None, :, :] == lengths[:, None, None]
    stream = hidden_in
    written = []
    for layer_index in range(LAYERS):
        normed = rms_scale(stream, norm_gains[layer_index, 0]).astype(jnp.bfloat16)
        projected = jnp.dot(normed, qkv_weight[layer_index].T, preferred_element_type=jnp.float32).astype(jnp.bfloat16)
        queries = rotate(projected[:, :q_cols].astype(jnp.float32).reshape(BATCH, HEADS, HEAD_DIM), lengths).astype(jnp.bfloat16)
        new_key = rotate(projected[:, q_cols:q_cols + k_cols].astype(jnp.float32).reshape(BATCH, KV_HEADS, HEAD_DIM), lengths).astype(jnp.bfloat16)
        new_value = projected[:, q_cols + k_cols:]
        key_layer = jnp.where(fresh_slot[:, :, :, None], new_key.reshape(BATCH, 1, 1, k_cols), ordered[layer_index, 0])
        value_layer = jnp.where(fresh_slot[:, :, :, None], new_value.reshape(BATCH, 1, 1, k_cols), ordered[layer_index, 1])
        written.append(jnp.stack([key_layer, value_layer], axis=0))
        shaped_q = queries.reshape(BATCH, KV_HEADS, head_share, HEAD_DIM).astype(jnp.float32)
        shaped_k = new_key.reshape(BATCH, KV_HEADS, 1, HEAD_DIM).astype(jnp.float32)
        shaped_v = new_value.reshape(BATCH, KV_HEADS, 1, HEAD_DIM).astype(jnp.float32)
        cached_keys = ordered[layer_index, 0].reshape(BATCH, N_TP, CTX_DEV, KV_HEADS, HEAD_DIM).astype(jnp.float32)
        cached_values = ordered[layer_index, 1].reshape(BATCH, N_TP, CTX_DEV, KV_HEADS, HEAD_DIM).astype(jnp.float32)
        raw_scores = jnp.einsum('bkmd,bjtkd->bkmjt', shaped_q, cached_keys) * score_scale
        weights = jnp.where(visible[:, None, None, :, :], jnp.exp(capped(raw_scores)), 0.0)
        own_weight = jnp.exp(capped(lax.optimization_barrier(jnp.sum(shaped_q * shaped_k, axis=-1)) * score_scale))
        denominator = lax.optimization_barrier(jnp.sum(weights, axis=(-2, -1))) + own_weight
        numerator = jnp.einsum('bkmjt,bjtkd->bkmd', round_back(weights), cached_values)
        numerator = numerator + round_back(own_weight)[..., None] * shaped_v
        attended = (numerator / denominator[..., None]).astype(jnp.bfloat16).reshape(BATCH, q_cols)
        mixed = jnp.dot(attended, out_weight[layer_index].T, preferred_element_type=jnp.float32).astype(jnp.bfloat16)
        stream = stream + rms_scale(mixed.astype(jnp.float32), norm_gains[layer_index, 1])
        ffn_in = rms_scale(stream, norm_gains[layer_index, 2]).astype(jnp.bfloat16)
        gate_proj = jnp.dot(ffn_in, gate_up_weight[layer_index, 0].T, preferred_element_type=jnp.float32)
        up_proj = jnp.dot(ffn_in, gate_up_weight[layer_index, 1].T, preferred_element_type=jnp.float32)
        active = (jax.nn.gelu(gate_proj, approximate=True) * up_proj).astype(jnp.bfloat16)
        branch = jnp.dot(active, down_weight[layer_index], preferred_element_type=jnp.float32)
        stream = stream + rms_scale(branch, norm_gains[layer_index, 3])
    decode_cache = jnp.stack(written, axis=0).transpose(3, 0, 1, 2, 4, 5)
    return (stream, decode_cache)
```

```python
import jax
import jax.numpy as jnp
from jax import lax
from jax.experimental import pallas as pl
from jax.experimental.pallas import tpu as pltpu
from jax.sharding import Mesh
from jax.sharding import PartitionSpec as P

D = 4608
HEADS = 32
KV_HEADS = 16
HEAD_DIM = 128
PREFILL_TP = 8
NX, NY, NC = 8, 8, 2
CHIPS = NX * NY
GROUP = CHIPS * NC
COLS = D // GROUP
TILE = 128
TILES = D // TILE
TP = ("tp_0", "tp_1", "tp_2")
MESH = pl.DeviceIdType.MESH
BF16 = jnp.bfloat16
F32 = jnp.float32

EPSILON = 1e-06
SOFTCAP = 50.0

A2A_POINTS = (16, 34, 50, 66, 84, 100, 116, 127)


def capped(raw_scores):
    return SOFTCAP * jnp.tanh(raw_scores / SOFTCAP)


def rms_scale(vector, gain_row):
    meansq = jnp.mean(vector * vector, axis=-1, keepdims=True)
    return vector * lax.rsqrt(meansq + EPSILON) * (1.0 + gain_row)


def dot_t(left, right):
    return lax.dot_general(left, right, (((1,), (1,)), ((), ())), preferred_element_type=F32)


def dot_n(left, right):
    return jnp.dot(left, right, preferred_element_type=F32)


def step_kernel(
    inv_ref, vis_ref, cos_ref, sin_ref, hid_hbm, paged_hbm, cache_hbm, wq_hbm, wo_hbm, wg_hbm, wd_hbm, gain_hbm,
    res_ref, nk_ref, nv_ref, dec_ref,
    hid, paged, cache, wq, wo, wg, wd, gain, arr, qs, qr, att_buf, att, mix_buf, mix, stream,
    br, pr, sb, rs_buf, fin, in_sem, own_sem, ss, rs,
):
    grp = lax.axis_index("grp")
    x = lax.axis_index("tp_0")
    y = lax.axis_index("tp_1")
    c = lax.axis_index("tp_2")
    chip = x * NY + y
    me = chip * NC + c
    my_group = lax.div(me, PREFILL_TP)
    my_slot = lax.rem(me, PREFILL_TP)

    def at(tx, ty, tc):
        return (grp, tx, ty, tc)

    barrier = pltpu.get_barrier_semaphore()

    def peer(i):
        tx = lax.rem(x + lax.div(i, NY * NC), NX)
        ty = lax.rem(y + lax.rem(lax.div(i, NC), NY), NY)
        tc = lax.rem(c + lax.rem(i, NC), NC)
        return tx, ty, tc

    def greet(i, carry):
        pl.semaphore_signal(barrier, inc=1, device_id=at(*peer(i)), device_id_type=MESH)
        return carry

    loads = [
        (hid_hbm, hid), (gain_hbm.at[0], gain), (wq_hbm.at[0], wq), (paged_hbm, paged),
        (wo_hbm.at[0], wo), (wg_hbm.at[0], wg), (wd_hbm.at[0], wd), (cache_hbm, cache),
    ]
    copies = [pltpu.make_async_copy(s, d, in_sem.at[n]) for n, (s, d) in enumerate(loads)]
    for copy in copies:
        copy.start()
    lax.fori_loop(1, GROUP, greet, 0)

    def send(src, dst, phase, target):
        pltpu.make_async_remote_copy(
            src_ref=src, dst_ref=dst, send_sem=ss.at[phase], recv_sem=rs.at[phase],
            device_id=target, device_id_type=MESH,
        ).start()

    def take(ref, sem):
        pltpu.make_async_copy(ref, ref, sem).wait()

    dec_mine = dec_ref.at[0, 0, :, pl.ds(my_group * 2, 2), :, pl.ds(pl.multiple_of(my_slot * 256, 256), 256)]

    def send_pages(first, last):
        def body(j, carry):
            tx, ty, tc = peer(lax.rem(j * 37, GROUP))
            send(arr.at[(tx * NY + ty) * NC + tc], dec_mine, 0, at(tx, ty, tc))
            return carry

        lax.fori_loop(first, last, body, 0)

    starts = (1,) + tuple(p + 1 for p in A2A_POINTS[:-1])
    stops = tuple(p + 1 for p in A2A_POINTS)

    def pages(n):
        send_pages(starts[n], stops[n])

    def spread(buf, phase):
        def body(i, carry):
            tx = lax.rem(x + lax.div(i, NY), NX)
            ty = lax.rem(y + lax.rem(i, NY), NY)
            send(buf.at[c, chip], buf.at[c, chip], phase, at(tx, ty, c))
            return carry

        lax.fori_loop(1, CHIPS, body, 0)

    def swap(buf, phase):
        send(buf.at[c], buf.at[c], phase, at(x, y, 1 - c))

    copies[0].wait()
    copies[1].wait()
    normed = rms_scale(hid[...], gain[0:1, :]).astype(BF16)
    copies[2].wait()
    part = dot_t(normed, wq[...]).astype(BF16).astype(F32)
    qs[...] = jnp.concatenate([part, part], axis=1).reshape(4, 8, TILE)

    copies[3].wait()

    def arrange(q, carry):
        for e in range(2):
            page = inv_ref[e, q]
            for kv in range(2):
                arr[q, kv, e] = paged[kv, e, page]
        return carry

    lax.fori_loop(0, GROUP, arrange, 0, unroll=4)
    pl.semaphore_wait(barrier, GROUP - 1)

    is_kv = lax.div(x, 4)
    xx = lax.rem(x, 2)
    ty4 = (1 - is_kv) * x + is_kv * (xx * 2 + lax.div(y, 4))
    tc4 = (1 - is_kv) * lax.div(y, 4) + is_kv * lax.rem(lax.div(y, 2), 2)
    slot = (1 - is_kv) * (lax.rem(y, 4) * 2 + c) + is_kv * (
        8 + lax.div(lax.rem(x, 4), 2) * 4 + lax.rem(y, 2) * 2 + c
    )

    def send_heads(i, carry):
        tx = lax.rem(x + lax.div(i, 2), NX)
        ty = ty4 + 4 * lax.rem(i, 2)
        mine = (tx == x) & (ty == y) & (tc4 == c)

        @pl.when(jnp.logical_not(mine))
        def _():
            send(qs.at[lax.div(tx, 2)], qr.at[slot], 1, at(tx, ty, tc4))

        @pl.when(mine)
        def _():
            qr[slot] = qs[lax.div(tx, 2)]

        return carry

    lax.fori_loop(0, 16, send_heads, 0)
    keeps_one = (lax.rem(y, 4) == ty4) & (tc4 == c)
    own_copy = pltpu.make_async_copy(arr.at[me], dec_mine, own_sem.at[0])
    own_copy.start()
    pages(0)

    @pl.when(keeps_one)
    def _():
        take(qr.at[pl.ds(0, 15)], rs.at[1])

    @pl.when(jnp.logical_not(keeps_one))
    def _():
        take(qr.at[pl.ds(0, 16)], rs.at[1])

    copies[7].wait()

    lane = lax.broadcasted_iota(jnp.int32, (8, TILE), 1)
    rows8 = lax.broadcasted_iota(jnp.int32, (8, TILE), 0)
    rows16 = lax.broadcasted_iota(jnp.int32, (16, TILE), 0)
    scale = (D / HEADS) ** (-0.5)
    message = jnp.zeros((16, TILE), F32)
    row0 = lax.rem(my_group, 4) * 2
    for e in range(2):
        cos = jnp.broadcast_to(cos_ref[e : e + 1, :], (8, TILE))
        sin = jnp.broadcast_to(sin_ref[e : e + 1, :], (8, TILE))

        def head(i):
            low = jnp.broadcast_to(qr[2 * i, pl.ds(row0 + e, 1), :], (8, TILE))
            high = jnp.broadcast_to(qr[2 * i + 1, pl.ds(row0 + e, 1), :], (8, TILE))
            return jnp.where(lane < HEAD_DIM // 2, low, high)

        def turned(u):
            return (u * cos + pltpu.roll(u, HEAD_DIM // 2, 1) * sin).astype(BF16).astype(F32)

        q = [turned(head(i)) for i in range(4)]
        k = [turned(head(4 + a)) for a in range(2)]
        v = [head(6 + a) for a in range(2)]
        zero = jnp.zeros((8, TILE), F32)
        left = jnp.where(rows8 == 0, q[0], jnp.where(rows8 == 1, q[1], zero))
        right = jnp.where(rows8 == 2, q[2], jnp.where(rows8 == 3, q[3], zero))
        own_raw = jnp.sum(left * k[0] + right * k[1], axis=1, keepdims=True) * scale
        own = jnp.exp(capped(own_raw))
        both = jnp.concatenate([left, right], axis=1).astype(BF16)
        raw = dot_t(both, cache[0, e]) * scale
        seen = jnp.broadcast_to(vis_ref[e : e + 1, :], raw.shape)
        weights = jnp.where(seen > 0.5, jnp.exp(capped(raw)), 0.0)
        den = jnp.sum(weights, axis=1, keepdims=True) + own
        num = dot_n(weights.astype(BF16), cache[1, e])
        own_b = own.astype(BF16).astype(F32)
        out_l = (num[:, :TILE] + own_b * v[0]) / den
        out_r = (num[:, TILE:] + own_b * v[1]) / den
        rows = [out_l[0:1], out_l[1:2], out_r[2:3], out_r[3:4], k[0][0:1], k[1][0:1], v[0][0:1], v[1][0:1]]
        for j, row in enumerate(rows):
            message = jnp.where(rows16 == e * 8 + j, jnp.broadcast_to(row, (16, TILE)), message)
    att_buf[c, chip] = message.astype(BF16)

    spread(att_buf, 2)
    pages(1)
    take(att_buf.at[0, pl.ds(0, CHIPS - 1)], rs.at[2])
    swap(att_buf, 3)
    take(att_buf.at[0], rs.at[3])

    want = lax.broadcasted_iota(jnp.int32, (128, 256), 0)
    have = lax.broadcasted_iota(jnp.int32, (128, 256), 1)
    target = 8 * lax.rem(want, 32) + lax.div(want, 32)
    pick_q = jnp.where(have == target, 1.0, 0.0).astype(BF16)
    pick_kv = jnp.where(have == target + 4, 1.0, 0.0).astype(BF16)

    def by_slot(k):
        return jnp.concatenate([att_buf[k % 2, 4 * g + k // 2] for g in range(16)], axis=0)

    for k in range(PREFILL_TP):
        picked = dot_n(pick_q, by_slot(k)).astype(BF16)
        for h in range(4):
            att[:, pl.ds((4 * k + h) * TILE, TILE)] = picked[32 * h : 32 * h + 32]
    copies[4].wait()
    mixed_part = dot_t(att[...], wo[...]).astype(BF16)
    shift = lax.rem(me * COLS, TILE)
    src_col = lax.broadcasted_iota(jnp.int32, (COLS, TILE), 0)
    dst_col = lax.broadcasted_iota(jnp.int32, (COLS, TILE), 1)
    put0 = jnp.where(dst_col == lax.rem(src_col + shift, TILE), 1.0, 0.0).astype(BF16)
    put1 = jnp.where(dst_col == lax.rem(src_col + shift + 64, TILE), 1.0, 0.0).astype(BF16)
    mix_buf[c, chip] = (dot_n(mixed_part[:16], put0) + dot_n(mixed_part[16:], put1)).astype(BF16)

    spread(mix_buf, 4)
    pages(2)
    for k in range(PREFILL_TP):
        picked = dot_n(pick_kv, by_slot(k)).astype(BF16)
        for a in range(2):
            nk_ref[:, pl.ds((2 * k + a) * TILE, TILE)] = picked[32 * a : 32 * a + 32]
            nv_ref[:, pl.ds((2 * k + a) * TILE, TILE)] = picked[64 + 32 * a : 96 + 32 * a]
    pages(3)
    take(mix_buf.at[0, pl.ds(0, CHIPS - 1)], rs.at[4])
    swap(mix_buf, 5)
    take(mix_buf.at[0], rs.at[5])

    lane16 = lax.broadcasted_iota(jnp.int32, (16, TILE), 1)

    def join(p, carry):
        straight, turned = [], []
        for i in range(32):
            piece = mix_buf[i % 2, p * 16 + i // 2].astype(F32)
            straight.append(piece)
            turned.append(pltpu.roll(piece, 64, 1))
        for t in range(9):
            top = bottom = None
            for i in range(32):
                lo, hi = COLS * i - TILE * t, COLS * i + COLS - TILE * t
                if hi <= 0 or lo >= TILE:
                    continue
                if top is None:
                    top, bottom = straight[i], turned[i]
                else:
                    later = lane16 >= lo
                    top = jnp.where(later, straight[i], top)
                    bottom = jnp.where(later, turned[i], bottom)
            column = pl.multiple_of((p * 9 + t) * TILE, TILE)
            mix[0:16, pl.ds(column, TILE)] = top
            mix[16:32, pl.ds(column, TILE)] = bottom
        return carry

    lax.fori_loop(0, 4, join, 0)
    stream[...] = hid[...] + rms_scale(mix[...], gain[1:2, :])
    ffn_in = rms_scale(stream[...], gain[2:3, :]).astype(BF16)
    copies[5].wait()
    gate = dot_t(ffn_in, wg[0])
    up = dot_t(ffn_in, wg[1])
    cube = gate + 0.044715 * (gate * gate * gate)
    active = (0.5 * gate * (1.0 + jnp.tanh(0.7978845608028654 * cube)) * up).astype(BF16)
    copies[6].wait()
    for n in range(4):
        columns = pl.ds(n * (D // 4), D // 4)
        piece = dot_n(active, wd[:, columns]).astype(BF16)
        br[0, :, columns] = piece[:16]
        br[1, :, columns] = piece[16:]

    send(br.at[1 - c], pr, 6, at(x, y, 1 - c))
    pages(4)
    take(pr, rs.at[6])
    sb[...] = (br[c].astype(F32) + pr[...].astype(F32)).astype(BF16)

    def send_sums(j, carry):
        owner = lax.div(j * 16, 9)
        tile = sb.at[:, pl.ds(pl.multiple_of(j * TILE, TILE), TILE)]

        @pl.when(owner != chip)
        def _():
            send(tile, rs_buf.at[chip], 7, at(lax.div(owner, NY), lax.rem(owner, NY), c))

        @pl.when(owner == chip)
        def _():
            rs_buf[chip] = tile[...]

        return carry

    lax.fori_loop(0, TILES, send_sums, 0)
    pages(5)
    my_tile = lax.div(chip * 9 + 15, 16)
    owns = lax.div(my_tile * 16, 9) == chip

    @pl.when(owns)
    def _():
        take(rs_buf.at[pl.ds(0, CHIPS - 1)], rs.at[7])
        total = jnp.zeros((16, TILE), F32)

        def add(i, acc):
            for n in range(8):
                acc = acc + rs_buf[i * 8 + n].astype(F32)
            return acc

        fin[c, my_tile] = lax.fori_loop(0, 8, add, total).astype(BF16)

        def tell(i, carry):
            tx = lax.rem(x + lax.div(i, NY), NX)
            ty = lax.rem(y + lax.rem(i, NY), NY)
            send(fin.at[c, my_tile], fin.at[c, my_tile], 8, at(tx, ty, c))
            return carry

        lax.fori_loop(1, CHIPS, tell, 0)

    pages(6)

    @pl.when(owns)
    def _():
        take(fin.at[0, pl.ds(0, TILES - 1)], rs.at[8])

    @pl.when(jnp.logical_not(owns))
    def _():
        take(fin.at[0, pl.ds(0, TILES)], rs.at[8])

    swap(fin, 9)
    pages(7)
    take(fin.at[0], rs.at[9])

    first = lax.div(me * COLS, TILE)
    second = jnp.minimum(first + 1, TILES - 1)
    for half in range(2):

        def square(j, acc):
            for n in range(4):
                tile = fin[half, j * 4 + n].astype(F32)
                acc = acc + tile * tile
            return acc

        squares = lax.fori_loop(0, TILES // 4, square, jnp.zeros((16, TILE), F32))
        factor = lax.rsqrt(jnp.sum(squares, axis=1, keepdims=True) / D + EPSILON)

        def block(t):
            columns = pl.ds(pl.multiple_of(t * TILE, TILE), TILE)
            branch = fin[half, t].astype(F32)
            value = stream[16 * half : 16 * half + 16, columns] + branch * factor * (1.0 + gain[3:4, columns])
            return pltpu.roll(value, lax.rem(TILE - shift, TILE), 1)

        res_ref[16 * half : 16 * half + 16, :] = jnp.where(lane16 < TILE - shift, block(first), block(second))

    own_copy.wait()
    take(arr.at[pl.ds(0, GROUP - 1)], rs.at[0])
    take(arr.at[pl.ds(0, GROUP - 1)], ss.at[0])

    @pl.when(keeps_one)
    def _():
        take(qr.at[pl.ds(0, 15)], ss.at[1])

    @pl.when(jnp.logical_not(keeps_one))
    def _():
        take(qr.at[pl.ds(0, 16)], ss.at[1])

    take(att_buf.at[0, pl.ds(0, CHIPS - 1)], ss.at[2])
    take(att_buf.at[0], ss.at[3])
    take(mix_buf.at[0, pl.ds(0, CHIPS - 1)], ss.at[4])
    take(mix_buf.at[0], ss.at[5])
    take(pr, ss.at[6])

    @pl.when(owns)
    def _():
        take(fin.at[0, pl.ds(0, TILES - 1)], ss.at[7])
        take(rs_buf.at[pl.ds(0, CHIPS - 1)], ss.at[8])

    @pl.when(jnp.logical_not(owns))
    def _():
        take(fin.at[0, pl.ds(0, TILES)], ss.at[7])

    take(fin.at[0], ss.at[9])


def on_device(
    hidden_in,
    prefill_cache,
    lengths,
    page_table,
    qkv_weight,
    out_weight,
    gate_up_weight,
    down_weight,
    norm_gains,
):
    me = lax.axis_index(TP)
    batch = hidden_in.shape[0]
    my_group = me // PREFILL_TP
    page_width = prefill_cache.shape[5]
    rows = lax.dynamic_slice_in_dim(page_table, my_group * 2, 2, 0)
    lens = lax.dynamic_slice_in_dim(lengths, my_group * 2, 2, 0)
    page_ids = jnp.arange(GROUP, dtype=jnp.int32)
    onehot = (rows[:, :, None] == page_ids[None, None, :]).astype(jnp.int32)
    inverse = jnp.sum(onehot * page_ids[None, :, None], axis=1)
    token = jnp.arange(page_width, dtype=jnp.int32)
    position = rows[:, :, None] * page_width + token[None, None, :]
    visible = (position < lens[:, None, None]).astype(F32).reshape(2, GROUP * page_width)
    half = HEAD_DIM // 2
    exponent = jnp.arange(half, dtype=F32) * (-2.0 / HEAD_DIM)
    angles = lens.astype(F32)[:, None] * jnp.power(jnp.float32(10000.0), exponent)
    cosine = jnp.cos(angles)
    sine = jnp.sin(angles)
    cos = jnp.concatenate([cosine, cosine], axis=1)
    sin = jnp.concatenate([-sine, sine], axis=1)
    paged = prefill_cache.reshape(2, 2, GROUP, page_width, 2 * HEAD_DIM)
    cache = prefill_cache.reshape(2, 2, GROUP * page_width, 2 * HEAD_DIM)
    k_cols = KV_HEADS * HEAD_DIM
    vmem = pl.BlockSpec(memory_space=pltpu.VMEM)
    hbm = pl.BlockSpec(memory_space=pl.ANY)
    dma = pltpu.SemaphoreType.DMA
    res, new_key, new_value, decoded = pl.pallas_call(
        step_kernel,
        name="step",
        out_shape=(
            jax.ShapeDtypeStruct((batch, TILE), F32),
            jax.ShapeDtypeStruct((batch, k_cols), BF16),
            jax.ShapeDtypeStruct((batch, k_cols), BF16),
            jax.ShapeDtypeStruct((1, 1, 2, batch, page_width, k_cols), BF16),
        ),
        in_specs=[pl.BlockSpec(memory_space=pltpu.SMEM)] + [vmem] * 3 + [hbm] * 8,
        out_specs=(vmem, vmem, vmem, hbm),
        scratch_shapes=[
            pltpu.VMEM((batch, D), F32),
            pltpu.VMEM(paged.shape, BF16),
            pltpu.VMEM(cache.shape, BF16),
            pltpu.VMEM(qkv_weight.shape[1:], BF16),
            pltpu.VMEM(out_weight.shape[1:], BF16),
            pltpu.VMEM(gate_up_weight.shape[1:], BF16),
            pltpu.VMEM(down_weight.shape[1:], BF16),
            pltpu.VMEM(norm_gains.shape[1:], F32),
            pltpu.VMEM((GROUP, 2, 2, page_width, 2 * HEAD_DIM), BF16),
            pltpu.VMEM((4, 8, TILE), F32),
            pltpu.VMEM((16, 8, TILE), F32),
            pltpu.VMEM((NC, CHIPS, 16, TILE), BF16),
            pltpu.VMEM((batch, HEADS * HEAD_DIM), BF16),
            pltpu.VMEM((NC, CHIPS, 16, TILE), BF16),
            pltpu.VMEM((batch, D), F32),
            pltpu.VMEM((batch, D), F32),
            pltpu.VMEM((2, 16, D), BF16),
            pltpu.VMEM((16, D), BF16),
            pltpu.VMEM((16, D), BF16),
            pltpu.VMEM((CHIPS, 16, TILE), BF16),
            pltpu.VMEM((NC, TILES, 16, TILE), BF16),
            dma((8,)),
            dma((1,)),
            dma((10,)),
            dma((10,)),
        ],
        compiler_params=pltpu.CompilerParams(
            collective_id=0, has_side_effects=True, vmem_limit_bytes=48 * 2**20
        ),
    )(inverse, visible, cos, sin, hidden_in, paged, cache, qkv_weight, out_weight, gate_up_weight, down_weight, norm_gains)
    my_pos = me * page_width + token
    fresh = (my_pos[None, :] == lengths[:, None])[None, None, None, :, :, None]
    new = jnp.stack([new_key, new_value], axis=0).reshape(1, 1, 2, batch, 1, k_cols)
    decode_cache = jnp.where(fresh, new, decoded)
    return (res[:, :COLS], decode_cache)


def solution(mesh):
    torus = Mesh(mesh.devices.reshape(mesh.shape["grp"], NX, NY, NC), ("grp",) + TP)
    return jax.shard_map(
        on_device,
        mesh=torus,
        in_specs=(
            P("grp", None),
            P(TP, None, None, "grp", None, None, None),
            P("grp"),
            P("grp", None),
            P(None, TP, None),
            P(None, TP, None),
            P(None, None, TP, None),
            P(None, TP, None),
            P(),
        ),
        out_specs=(P("grp", TP), P(TP, None, None, "grp", None, None)),
        check_vma=False,
    )
```

```python
import jax
import jax.numpy as jnp
import numpy as np
from jax import lax
from jax.experimental import pallas as pl
from jax.experimental.pallas import tpu as pltpu
from jax.sharding import Mesh
from jax.sharding import PartitionSpec as P

D = 4608
HEADS = 32
KV_HEADS = 16
HEAD_DIM = 128
PREFILL_TP = 8
NX, NY, NC = 8, 8, 2
CHIPS = NX * NY
GROUP = CHIPS * NC
COLS = D // GROUP
TILE = 128
TILES = D // TILE
TP = ("tp_0", "tp_1", "tp_2")
MESH = pl.DeviceIdType.MESH
BF16 = jnp.bfloat16
F32 = jnp.float32

EPSILON = 1e-06
SOFTCAP = 50.0

PAGES = (24, 24, 18, 12, 24, 25)


def capped(raw_scores):
    return SOFTCAP * jnp.tanh(raw_scores / SOFTCAP)


def rms_scale(vector, gain_row):
    meansq = jnp.mean(vector * vector, axis=-1, keepdims=True)
    return vector * lax.rsqrt(meansq + EPSILON) * (1.0 + gain_row)


def dot_t(left, right):
    return lax.dot_general(left, right, (((1,), (1,)), ((), ())), preferred_element_type=F32)


def dot_n(left, right):
    return jnp.dot(left, right, preferred_element_type=F32)


def step_kernel(
    len_ref, table_hbm, freq_hbm, hid_hbm, paged_hbm, cache_hbm, wq_hbm, wo_hbm, wg_hbm, wd_hbm, gain_hbm,
    res_ref, nk_ref, nv_ref, dec_ref,
    table, freq, inv_v, inv, hid, paged, cache, wq, wo, wg, wd, gain, arr, qs, qr, att_buf, att, mix_buf, mix, stream,
    br, pr, sb, rs_buf, fin, in_sem, own_sem, ss, rs,
):
    grp = lax.axis_index("grp")
    x = lax.axis_index("tp_0")
    y = lax.axis_index("tp_1")
    c = lax.axis_index("tp_2")
    chip = x * NY + y
    me = chip * NC + c
    my_group = lax.div(me, PREFILL_TP)
    my_slot = lax.rem(me, PREFILL_TP)

    def at(tx, ty, tc):
        return (grp, tx, ty, tc)

    barrier = pltpu.get_barrier_semaphore()

    def peer(i):
        tx = lax.rem(x + lax.div(i, NY * NC), NX)
        ty = lax.rem(y + lax.rem(lax.div(i, NC), NY), NY)
        tc = lax.rem(c + lax.rem(i, NC), NC)
        return tx, ty, tc

    def greet(i, carry):
        pl.semaphore_signal(barrier, inc=1, device_id=at(*peer(i)), device_id_type=MESH)
        return carry

    loads = [
        (table_hbm, table), (freq_hbm, freq), (hid_hbm, hid),
        (gain_hbm.at[0], gain), (wq_hbm.at[0], wq), (paged_hbm, paged),
        (wo_hbm.at[0], wo), (wg_hbm.at[0], wg), (wd_hbm.at[0], wd), (cache_hbm, cache),
    ]
    copies = [pltpu.make_async_copy(s, d, in_sem.at[n]) for n, (s, d) in enumerate(loads)]
    for copy in copies:
        copy.start()
    lax.fori_loop(1, GROUP, greet, 0)

    def send(src, dst, phase, target):
        pltpu.make_async_remote_copy(
            src_ref=src, dst_ref=dst, send_sem=ss.at[phase], recv_sem=rs.at[phase],
            device_id=target, device_id_type=MESH,
        ).start()

    def take(ref, sem):
        pltpu.make_async_copy(ref, ref, sem).wait()

    dec_mine = dec_ref.at[0, 0, :, pl.ds(my_group * 2, 2), :, pl.ds(pl.multiple_of(my_slot * 256, 256), 256)]

    def send_pages(first, last):
        def body(j, carry):
            tx, ty, tc = peer(lax.rem(j * 37, GROUP))
            send(arr.at[(tx * NY + ty) * NC + tc], dec_mine, 0, at(tx, ty, tc))
            return carry

        lax.fori_loop(first, last, body, 0)

    def pages(n):
        first = 1 + sum(PAGES[:n])
        send_pages(first, first + PAGES[n])

    def other_chip(i):
        n = i + lax.div(i, 36)
        tx = lax.rem(x + 4 + lax.div(n, NY), NX)
        ty = lax.rem(y + 4 + lax.rem(n, NY), NY)
        return tx, ty

    def spread(buf, phase):
        def body(i, carry):
            tx, ty = other_chip(i)
            send(buf.at[c, chip], buf.at[c, chip], phase, at(tx, ty, c))
            return carry

        lax.fori_loop(0, CHIPS - 1, body, 0)

    def swap(buf, phase):
        send(buf.at[c], buf.at[c], phase, at(x, y, 1 - c))

    copies[2].wait()
    copies[3].wait()
    normed = rms_scale(hid[...], gain[0:1, :]).astype(BF16)
    copies[4].wait()
    part = dot_t(normed, wq[...]).astype(BF16).astype(F32)
    qs[...] = jnp.concatenate([part, part], axis=1).reshape(4, 8, TILE)

    copies[0].wait()
    block = lax.broadcasted_iota(jnp.int32, (GROUP, GROUP), 0)
    index = lax.broadcasted_iota(jnp.int32, (8, GROUP), 1).astype(F32).astype(BF16)
    tables = []
    for e in range(2):
        row = table[pl.ds(my_group * 2 + e, 1), :]
        tables.append(row)
        hits = jnp.where(jnp.broadcast_to(row, (GROUP, GROUP)) == block, 1.0, 0.0).astype(BF16)
        inv_v[8 * e : 8 * e + 8, :] = dot_t(index, hits).astype(jnp.int32)
    to_scalars = pltpu.make_async_copy(inv_v, inv, own_sem.at[1])
    to_scalars.start()

    copies[1].wait()
    slot_page = lax.broadcasted_iota(jnp.int32, (GROUP, GROUP * 8), 0)
    slot_at = lax.broadcasted_iota(jnp.int32, (GROUP, GROUP * 8), 1)
    widen = jnp.where(lax.div(slot_at, 8) == slot_page, 1.0, 0.0).astype(BF16)
    token = lax.rem(lax.broadcasted_iota(jnp.int32, (8, GROUP * 8), 1), 8).astype(F32)
    lane = lax.broadcasted_iota(jnp.int32, (8, TILE), 1)
    seen, cosines, sines = [], [], []
    for e in range(2):
        length = len_ref[my_group * 2 + e].astype(F32)
        row = jnp.broadcast_to(tables[e], (8, GROUP)).astype(F32).astype(BF16)
        seen.append(dot_n(row, widen) * 8.0 + token < length)
        angle = jnp.broadcast_to(freq[...], (8, TILE)) * length
        sine = jnp.sin(angle)
        cosines.append(jnp.cos(angle))
        sines.append(jnp.where(lane < HEAD_DIM // 2, -sine, sine))

    copies[5].wait()
    to_scalars.wait()

    def arrange(q, carry):
        for e in range(2):
            page = jnp.maximum(jnp.minimum(inv[8 * e, q], GROUP - 1), 0)
            for kv in range(2):
                arr[q, kv, e] = paged[kv, e, page]
        return carry

    lax.fori_loop(0, GROUP, arrange, 0, unroll=4)
    pl.semaphore_wait(barrier, GROUP - 1)

    is_kv = lax.div(x, 4)
    xx = lax.rem(x, 2)
    ty4 = (1 - is_kv) * x + is_kv * (xx * 2 + lax.div(y, 4))
    tc4 = (1 - is_kv) * lax.div(y, 4) + is_kv * lax.rem(lax.div(y, 2), 2)
    slot = (1 - is_kv) * (lax.rem(y, 4) * 2 + c) + is_kv * (
        8 + lax.div(lax.rem(x, 4), 2) * 4 + lax.rem(y, 2) * 2 + c
    )

    def send_heads(i, carry):
        tx = lax.rem(x + lax.div(i, 2), NX)
        ty = ty4 + 4 * lax.rem(i, 2)
        mine = (tx == x) & (ty == y) & (tc4 == c)

        @pl.when(jnp.logical_not(mine))
        def _():
            send(qs.at[lax.div(tx, 2)], qr.at[slot], 1, at(tx, ty, tc4))

        @pl.when(mine)
        def _():
            qr[slot] = qs[lax.div(tx, 2)]

        return carry

    lax.fori_loop(0, 16, send_heads, 0)
    keeps_one = (lax.rem(y, 4) == ty4) & (tc4 == c)
    own_copy = pltpu.make_async_copy(arr.at[me], dec_mine, own_sem.at[0])
    own_copy.start()
    pages(0)

    @pl.when(keeps_one)
    def _():
        take(qr.at[pl.ds(0, 15)], rs.at[1])

    @pl.when(jnp.logical_not(keeps_one))
    def _():
        take(qr.at[pl.ds(0, 16)], rs.at[1])

    copies[9].wait()

    rows8 = lax.broadcasted_iota(jnp.int32, (8, TILE), 0)
    rows16 = lax.broadcasted_iota(jnp.int32, (16, TILE), 0)
    scale = (D / HEADS) ** (-0.5)
    message = jnp.zeros((16, TILE), F32)
    row0 = lax.rem(my_group, 4) * 2
    for e in range(2):
        cos, sin = cosines[e], sines[e]

        def head(i):
            low = jnp.broadcast_to(qr[2 * i, pl.ds(row0 + e, 1), :], (8, TILE))
            high = jnp.broadcast_to(qr[2 * i + 1, pl.ds(row0 + e, 1), :], (8, TILE))
            return jnp.where(lane < HEAD_DIM // 2, low, high)

        def turned(u):
            return (u * cos + pltpu.roll(u, HEAD_DIM // 2, 1) * sin).astype(BF16).astype(F32)

        q = [turned(head(i)) for i in range(4)]
        k = [turned(head(4 + a)) for a in range(2)]
        v = [head(6 + a) for a in range(2)]
        zero = jnp.zeros((8, TILE), F32)
        left = jnp.where(rows8 == 0, q[0], jnp.where(rows8 == 1, q[1], zero))
        right = jnp.where(rows8 == 2, q[2], jnp.where(rows8 == 3, q[3], zero))
        own_raw = jnp.sum(left * k[0] + right * k[1], axis=1, keepdims=True) * scale
        own = jnp.exp(capped(own_raw))
        both = jnp.concatenate([left, right], axis=1).astype(BF16)
        raw = dot_t(both, cache[0, e]) * scale
        weights = jnp.where(seen[e], jnp.exp(capped(raw)), 0.0)
        den = jnp.sum(weights, axis=1, keepdims=True) + own
        num = dot_n(weights.astype(BF16), cache[1, e])
        own_b = own.astype(BF16).astype(F32)
        out_l = (num[:, :TILE] + own_b * v[0]) / den
        out_r = (num[:, TILE:] + own_b * v[1]) / den
        rows = [out_l[0:1], out_l[1:2], out_r[2:3], out_r[3:4], k[0][0:1], k[1][0:1], v[0][0:1], v[1][0:1]]
        for j, row in enumerate(rows):
            message = jnp.where(rows16 == e * 8 + j, jnp.broadcast_to(row, (16, TILE)), message)
    att_buf[c, chip] = message.astype(BF16)

    spread(att_buf, 2)
    pages(1)
    take(att_buf.at[0, pl.ds(0, CHIPS - 1)], rs.at[2])
    swap(att_buf, 3)
    take(att_buf.at[0], rs.at[3])

    want = lax.broadcasted_iota(jnp.int32, (128, 256), 0)
    have = lax.broadcasted_iota(jnp.int32, (128, 256), 1)
    target = 8 * lax.rem(want, 32) + lax.div(want, 32)
    pick_q = jnp.where(have == target, 1.0, 0.0).astype(BF16)
    pick_kv = jnp.where(have == target + 4, 1.0, 0.0).astype(BF16)

    def by_slot(k):
        return jnp.concatenate([att_buf[k % 2, 4 * g + k // 2] for g in range(16)], axis=0)

    for k in range(PREFILL_TP):
        picked = dot_n(pick_q, by_slot(k)).astype(BF16)
        for h in range(4):
            att[:, pl.ds((4 * k + h) * TILE, TILE)] = picked[32 * h : 32 * h + 32]
    copies[6].wait()
    mixed_part = dot_t(att[...], wo[...]).astype(BF16)
    shift = lax.rem(me * COLS, TILE)
    src_col = lax.broadcasted_iota(jnp.int32, (COLS, TILE), 0)
    dst_col = lax.broadcasted_iota(jnp.int32, (COLS, TILE), 1)
    put0 = jnp.where(dst_col == lax.rem(src_col + shift, TILE), 1.0, 0.0).astype(BF16)
    put1 = jnp.where(dst_col == lax.rem(src_col + shift + 64, TILE), 1.0, 0.0).astype(BF16)
    mix_buf[c, chip] = (dot_n(mixed_part[:16], put0) + dot_n(mixed_part[16:], put1)).astype(BF16)

    spread(mix_buf, 4)
    pages(2)
    for k in range(PREFILL_TP):
        picked = dot_n(pick_kv, by_slot(k)).astype(BF16)
        for a in range(2):
            nk_ref[:, pl.ds((2 * k + a) * TILE, TILE)] = picked[32 * a : 32 * a + 32]
            nv_ref[:, pl.ds((2 * k + a) * TILE, TILE)] = picked[64 + 32 * a : 96 + 32 * a]
    pages(3)
    take(mix_buf.at[0, pl.ds(0, CHIPS - 1)], rs.at[4])
    swap(mix_buf, 5)
    take(mix_buf.at[0], rs.at[5])

    lane16 = lax.broadcasted_iota(jnp.int32, (16, TILE), 1)

    def join(p, carry):
        straight, turned = [], []
        for i in range(32):
            piece = mix_buf[i % 2, p * 16 + i // 2].astype(F32)
            straight.append(piece)
            turned.append(pltpu.roll(piece, 64, 1))
        for t in range(9):
            top = bottom = None
            for i in range(32):
                lo, hi = COLS * i - TILE * t, COLS * i + COLS - TILE * t
                if hi <= 0 or lo >= TILE:
                    continue
                if top is None:
                    top, bottom = straight[i], turned[i]
                else:
                    later = lane16 >= lo
                    top = jnp.where(later, straight[i], top)
                    bottom = jnp.where(later, turned[i], bottom)
            column = pl.multiple_of((p * 9 + t) * TILE, TILE)
            mix[0:16, pl.ds(column, TILE)] = top
            mix[16:32, pl.ds(column, TILE)] = bottom
        return carry

    lax.fori_loop(0, 4, join, 0)
    stream[...] = hid[...] + rms_scale(mix[...], gain[1:2, :])
    ffn_in = rms_scale(stream[...], gain[2:3, :]).astype(BF16)
    copies[7].wait()
    gate = dot_t(ffn_in, wg[0])
    up = dot_t(ffn_in, wg[1])
    cube = gate + 0.044715 * (gate * gate * gate)
    active = (0.5 * gate * (1.0 + jnp.tanh(0.7978845608028654 * cube)) * up).astype(BF16)
    copies[8].wait()
    for n in range(4):
        columns = pl.ds(n * (D // 4), D // 4)
        piece = dot_n(active, wd[:, columns]).astype(BF16)
        br[0, :, columns] = piece[:16]
        br[1, :, columns] = piece[16:]

    send(br.at[1 - c], pr, 6, at(x, y, 1 - c))
    take(pr, rs.at[6])
    sb[...] = (br[c].astype(F32) + pr[...].astype(F32)).astype(BF16)

    def send_sums(j, carry):
        owner = lax.div(j * 16, 9)
        tile = sb.at[:, pl.ds(pl.multiple_of(j * TILE, TILE), TILE)]

        @pl.when(owner != chip)
        def _():
            send(tile, rs_buf.at[chip], 7, at(lax.div(owner, NY), lax.rem(owner, NY), c))

        @pl.when(owner == chip)
        def _():
            rs_buf[chip] = tile[...]

        return carry

    lax.fori_loop(0, TILES, send_sums, 0)
    pages(4)
    my_tile = lax.div(chip * 9 + 15, 16)
    owns = lax.div(my_tile * 16, 9) == chip

    @pl.when(owns)
    def _():
        take(rs_buf.at[pl.ds(0, CHIPS - 1)], rs.at[7])
        total = jnp.zeros((16, TILE), F32)

        def add(i, acc):
            for n in range(8):
                acc = acc + rs_buf[i * 8 + n].astype(F32)
            return acc

        fin[c, my_tile] = lax.fori_loop(0, 8, add, total).astype(BF16)

        def tell(i, carry):
            tx, ty = other_chip(i)
            send(fin.at[c, my_tile], fin.at[c, my_tile], 8, at(tx, ty, c))
            return carry

        lax.fori_loop(0, CHIPS - 1, tell, 0)

    pages(5)

    @pl.when(owns)
    def _():
        take(fin.at[0, pl.ds(0, TILES - 1)], rs.at[8])

    @pl.when(jnp.logical_not(owns))
    def _():
        take(fin.at[0, pl.ds(0, TILES)], rs.at[8])

    swap(fin, 9)
    take(fin.at[0], rs.at[9])

    first = lax.div(me * COLS, TILE)
    second = jnp.minimum(first + 1, TILES - 1)
    for half in range(2):

        def square(j, acc):
            for n in range(4):
                tile = fin[half, j * 4 + n].astype(F32)
                acc = acc + tile * tile
            return acc

        squares = lax.fori_loop(0, TILES // 4, square, jnp.zeros((16, TILE), F32))
        factor = lax.rsqrt(jnp.sum(squares, axis=1, keepdims=True) / D + EPSILON)

        def block(t):
            columns = pl.ds(pl.multiple_of(t * TILE, TILE), TILE)
            branch = fin[half, t].astype(F32)
            value = stream[16 * half : 16 * half + 16, columns] + branch * factor * (1.0 + gain[3:4, columns])
            return pltpu.roll(value, lax.rem(TILE - shift, TILE), 1)

        res_ref[16 * half : 16 * half + 16, :] = jnp.where(lane16 < TILE - shift, block(first), block(second))

    own_copy.wait()
    take(arr.at[pl.ds(0, GROUP - 1)], rs.at[0])
    take(arr.at[pl.ds(0, GROUP - 1)], ss.at[0])

    @pl.when(keeps_one)
    def _():
        take(qr.at[pl.ds(0, 15)], ss.at[1])

    @pl.when(jnp.logical_not(keeps_one))
    def _():
        take(qr.at[pl.ds(0, 16)], ss.at[1])

    take(att_buf.at[0, pl.ds(0, CHIPS - 1)], ss.at[2])
    take(att_buf.at[0], ss.at[3])
    take(mix_buf.at[0, pl.ds(0, CHIPS - 1)], ss.at[4])
    take(mix_buf.at[0], ss.at[5])
    take(pr, ss.at[6])

    @pl.when(owns)
    def _():
        take(fin.at[0, pl.ds(0, TILES - 1)], ss.at[7])
        take(rs_buf.at[pl.ds(0, CHIPS - 1)], ss.at[8])

    @pl.when(jnp.logical_not(owns))
    def _():
        take(fin.at[0, pl.ds(0, TILES)], ss.at[7])

    take(fin.at[0], ss.at[9])


def on_device(
    hidden_in,
    prefill_cache,
    lengths,
    page_table,
    qkv_weight,
    out_weight,
    gate_up_weight,
    down_weight,
    norm_gains,
):
    me = lax.axis_index(TP)
    batch = hidden_in.shape[0]
    page_width = prefill_cache.shape[5]
    exponent = np.arange(HEAD_DIM // 2, dtype=np.float32) * np.float32(-2.0 / HEAD_DIM)
    frequency = np.power(np.float32(10000.0), exponent).astype(np.float32)
    frequency = jnp.asarray(np.concatenate([frequency, frequency])[None, :])
    paged = prefill_cache.reshape(2, 2, GROUP, page_width, 2 * HEAD_DIM)
    cache = prefill_cache.reshape(2, 2, GROUP * page_width, 2 * HEAD_DIM)
    k_cols = KV_HEADS * HEAD_DIM
    vmem = pl.BlockSpec(memory_space=pltpu.VMEM)
    hbm = pl.BlockSpec(memory_space=pltpu.HBM)
    dma = pltpu.SemaphoreType.DMA
    res, new_key, new_value, decoded = pl.pallas_call(
        step_kernel,
        name="step",
        out_shape=(
            jax.ShapeDtypeStruct((batch, TILE), F32),
            jax.ShapeDtypeStruct((batch, k_cols), BF16),
            jax.ShapeDtypeStruct((batch, k_cols), BF16),
            jax.ShapeDtypeStruct((1, 1, 2, batch, page_width, k_cols), BF16),
        ),
        in_specs=[pl.BlockSpec(memory_space=pltpu.SMEM)] + [hbm] * 10,
        out_specs=(vmem, vmem, vmem, pl.BlockSpec(memory_space=pl.ANY)),
        scratch_shapes=[
            pltpu.VMEM(page_table.shape, jnp.int32),
            pltpu.VMEM(frequency.shape, F32),
            pltpu.VMEM((16, GROUP), jnp.int32),
            pltpu.SMEM((16, GROUP), jnp.int32),
            pltpu.VMEM((batch, D), F32),
            pltpu.VMEM(paged.shape, BF16),
            pltpu.VMEM(cache.shape, BF16),
            pltpu.VMEM(qkv_weight.shape[1:], BF16),
            pltpu.VMEM(out_weight.shape[1:], BF16),
            pltpu.VMEM(gate_up_weight.shape[1:], BF16),
            pltpu.VMEM(down_weight.shape[1:], BF16),
            pltpu.VMEM(norm_gains.shape[1:], F32),
            pltpu.VMEM((GROUP, 2, 2, page_width, 2 * HEAD_DIM), BF16),
            pltpu.VMEM((4, 8, TILE), F32),
            pltpu.VMEM((16, 8, TILE), F32),
            pltpu.VMEM((NC, CHIPS, 16, TILE), BF16),
            pltpu.VMEM((batch, HEADS * HEAD_DIM), BF16),
            pltpu.VMEM((NC, CHIPS, 16, TILE), BF16),
            pltpu.VMEM((batch, D), F32),
            pltpu.VMEM((batch, D), F32),
            pltpu.VMEM((2, 16, D), BF16),
            pltpu.VMEM((16, D), BF16),
            pltpu.VMEM((16, D), BF16),
            pltpu.VMEM((CHIPS, 16, TILE), BF16),
            pltpu.VMEM((NC, TILES, 16, TILE), BF16),
            dma((10,)),
            dma((2,)),
            dma((10,)),
            dma((10,)),
        ],
        compiler_params=pltpu.CompilerParams(
            collective_id=0, has_side_effects=True, vmem_limit_bytes=67043328
        ),
    )(lengths, page_table, frequency, hidden_in, paged, cache, qkv_weight, out_weight, gate_up_weight, down_weight, norm_gains)
    my_pos = me * page_width + jnp.arange(page_width, dtype=jnp.int32)
    fresh = (my_pos[None, :] == lengths[:, None])[None, None, None, :, :, None]
    new = jnp.stack([new_key, new_value], axis=0).reshape(1, 1, 2, batch, 1, k_cols)
    decode_cache = jnp.where(fresh, new, decoded)
    return (res[:, :COLS], decode_cache)


def solution(mesh):
    torus = Mesh(mesh.devices.reshape(mesh.shape["grp"], NX, NY, NC), ("grp",) + TP)
    return jax.shard_map(
        on_device,
        mesh=torus,
        in_specs=(
            P("grp", None),
            P(TP, None, None, "grp", None, None, None),
            P("grp"),
            P("grp", None),
            P(None, TP, None),
            P(None, TP, None),
            P(None, None, TP, None),
            P(None, TP, None),
            P(),
        ),
        out_specs=(P("grp", TP), P(TP, None, None, "grp", None, None)),
        check_vma=False,
    )
```

```python
import jax
import jax.numpy as jnp
import numpy as np
from jax import lax
from jax.experimental import pallas as pl
from jax.experimental.pallas import tpu as pltpu
from jax.sharding import Mesh
from jax.sharding import PartitionSpec as P

D = 4608
HEADS = 32
KV_HEADS = 16
HEAD_DIM = 128
PREFILL_TP = 8
NX, NY, NC = 8, 8, 2
CHIPS = NX * NY
GROUP = CHIPS * NC
COLS = D // GROUP
TILE = 128
TILES = D // TILE
TP = ("tp_0", "tp_1", "tp_2")
MESH = pl.DeviceIdType.MESH
BF16 = jnp.bfloat16
F32 = jnp.float32

EPSILON = 1e-06
SOFTCAP = 50.0

PAGES = (24, 12, 18, 12, 18, 20, 23)


def capped(raw_scores):
    return SOFTCAP * jnp.tanh(raw_scores / SOFTCAP)


def rms_scale(vector, gain_row):
    meansq = jnp.mean(vector * vector, axis=-1, keepdims=True)
    return vector * lax.rsqrt(meansq + EPSILON) * (1.0 + gain_row)


def dot_t(left, right):
    return lax.dot_general(left, right, (((1,), (1,)), ((), ())), preferred_element_type=F32)


def dot_n(left, right):
    return jnp.dot(left, right, preferred_element_type=F32)


def step_kernel(
    len_ref, table_hbm, freq_hbm, hid_hbm, paged_hbm, cache_hbm, wq_hbm, wo_hbm, wg_hbm, wd_hbm, gain_hbm,
    res_ref, nk_ref, nv_ref, dec_ref,
    table, freq, inv_v, inv, hid, paged, cache, wq, wo, wg, wd, gain, arr, qs, qr, qf, att_buf, att, mix_buf, mix, stream,
    br, pr, sb, rs_buf, fin, in_sem, own_sem, ss, rs,
):
    grp = lax.axis_index("grp")
    x = lax.axis_index("tp_0")
    y = lax.axis_index("tp_1")
    c = lax.axis_index("tp_2")
    chip = x * NY + y
    me = chip * NC + c
    my_group = lax.div(me, PREFILL_TP)
    my_slot = lax.rem(me, PREFILL_TP)

    def at(tx, ty, tc):
        return (grp, tx, ty, tc)

    barrier = pltpu.get_barrier_semaphore()

    def peer(i):
        tx = lax.rem(x + lax.div(i, NY * NC), NX)
        ty = lax.rem(y + lax.rem(lax.div(i, NC), NY), NY)
        tc = lax.rem(c + lax.rem(i, NC), NC)
        return tx, ty, tc

    def greet(i, carry):
        pl.semaphore_signal(barrier, inc=1, device_id=at(*peer(i)), device_id_type=MESH)
        return carry

    loads = [
        (table_hbm, table), (freq_hbm, freq), (hid_hbm, hid),
        (gain_hbm.at[0], gain), (wq_hbm.at[0], wq), (paged_hbm, paged),
        (wo_hbm.at[0], wo), (wg_hbm.at[0], wg), (wd_hbm.at[0], wd), (cache_hbm, cache),
    ]
    copies = [pltpu.make_async_copy(s, d, in_sem.at[n]) for n, (s, d) in enumerate(loads)]
    for copy in copies:
        copy.start()
    lax.fori_loop(1, GROUP, greet, 0)

    def send(src, dst, phase, target):
        pltpu.make_async_remote_copy(
            src_ref=src, dst_ref=dst, send_sem=ss.at[phase], recv_sem=rs.at[phase],
            device_id=target, device_id_type=MESH,
        ).start()

    def take(ref, sem):
        pltpu.make_async_copy(ref, ref, sem).wait()

    dec_mine = dec_ref.at[0, 0, :, pl.ds(my_group * 2, 2), :, pl.ds(pl.multiple_of(my_slot * 256, 256), 256)]

    def send_pages(first, last):
        def body(j, carry):
            tx, ty, tc = peer(lax.rem(j * 37, GROUP))
            send(arr.at[(tx * NY + ty) * NC + tc], dec_mine, 0, at(tx, ty, tc))
            return carry

        lax.fori_loop(first, last, body, 0)

    def pages(n):
        first = 1 + sum(PAGES[:n])
        send_pages(first, first + PAGES[n])

    def other_chip(i):
        n = i + lax.div(i, 36)
        tx = lax.rem(x + 4 + lax.div(n, NY), NX)
        ty = lax.rem(y + 4 + lax.rem(n, NY), NY)
        return tx, ty

    x2, xp, y2, yp = lax.div(x, 2), lax.rem(x, 2), lax.div(y, 2), lax.rem(y, 2)
    even = 1 - lax.rem(x + y, 2)

    def mine(buf):
        return buf.at[c, x2, xp, y2, yp]

    def first_leg(buf, phase):
        for o in (4, 3, 5, 2, 6, 1, 7):
            target = at(lax.rem(x + even * o, NX), lax.rem(y + (1 - even) * o, NY), c)
            send(mine(buf), mine(buf), phase, target)

    def second_leg(buf, phase):
        take(rs_buf.at[pl.ds(0, 7)], rs.at[phase])
        row = buf.at[c, :, yp, y2, yp]
        column = buf.at[c, x2, xp, :, 1 - xp]
        for o in (4, 3, 5, 2, 6, 1, 7):
            send(row, row, phase + 1, at(x, lax.rem(y + o, NY), c))
            send(column, column, phase + 1, at(lax.rem(x + o, NX), y, c))

    def last_leg(buf, phase):
        take(rs_buf.at[pl.ds(0, 56)], rs.at[phase + 1])
        swap(buf, phase + 2)
        take(buf.at[0], rs.at[phase + 2])

    def gone(buf, phase):
        take(rs_buf.at[pl.ds(0, 7)], ss.at[phase])
        take(rs_buf.at[pl.ds(0, 56)], ss.at[phase + 1])
        take(buf.at[0], ss.at[phase + 2])

    def swap(buf, phase):
        send(buf.at[c], buf.at[c], phase, at(x, y, 1 - c))

    copies[2].wait()
    copies[3].wait()
    normed = rms_scale(hid[...], gain[0:1, :]).astype(BF16)
    copies[4].wait()
    part = dot_t(normed, wq[...]).astype(BF16)
    part = jnp.concatenate([part, part], axis=1)
    for t in range(4):
        qs[t] = part[8 * t : 8 * t + 8]

    copies[0].wait()
    block = lax.broadcasted_iota(jnp.int32, (GROUP, GROUP), 0)
    index = lax.broadcasted_iota(jnp.int32, (8, GROUP), 1).astype(F32).astype(BF16)
    tables = []
    for e in range(2):
        row = table[pl.ds(my_group * 2 + e, 1), :]
        tables.append(row)
        hits = jnp.where(jnp.broadcast_to(row, (GROUP, GROUP)) == block, 1.0, 0.0).astype(BF16)
        inv_v[8 * e : 8 * e + 8, :] = dot_t(index, hits).astype(jnp.int32)
    to_scalars = pltpu.make_async_copy(inv_v, inv, own_sem.at[1])
    to_scalars.start()

    copies[1].wait()
    slot_page = lax.broadcasted_iota(jnp.int32, (GROUP, GROUP * 8), 0)
    slot_at = lax.broadcasted_iota(jnp.int32, (GROUP, GROUP * 8), 1)
    widen = jnp.where(lax.div(slot_at, 8) == slot_page, 1.0, 0.0).astype(BF16)
    token = lax.rem(lax.broadcasted_iota(jnp.int32, (8, GROUP * 8), 1), 8).astype(F32)
    lane = lax.broadcasted_iota(jnp.int32, (8, TILE), 1)
    seen, cosines, sines = [], [], []
    for e in range(2):
        length = len_ref[my_group * 2 + e].astype(F32)
        row = jnp.broadcast_to(tables[e], (8, GROUP)).astype(F32).astype(BF16)
        seen.append(dot_n(row, widen) * 8.0 + token < length)
        angle = jnp.broadcast_to(freq[...], (8, TILE)) * length
        sine = jnp.sin(angle)
        cosines.append(jnp.cos(angle))
        sines.append(jnp.where(lane < HEAD_DIM // 2, -sine, sine))

    copies[5].wait()
    to_scalars.wait()

    def arrange(q, carry):
        for e in range(2):
            page = jnp.maximum(jnp.minimum(inv[8 * e, q], GROUP - 1), 0)
            for kv in range(2):
                arr[q, kv, e] = paged[kv, e, page]
        return carry

    lax.fori_loop(0, GROUP, arrange, 0, unroll=4)
    pl.semaphore_wait(barrier, GROUP - 1)

    is_kv = lax.div(x, 4)
    xx = lax.rem(x, 2)
    ty4 = (1 - is_kv) * x + is_kv * (xx * 2 + lax.div(y, 4))
    tc4 = (1 - is_kv) * lax.div(y, 4) + is_kv * lax.rem(lax.div(y, 2), 2)
    slot = (1 - is_kv) * (lax.rem(y, 4) * 2 + c) + is_kv * (
        8 + lax.div(lax.rem(x, 4), 2) * 4 + lax.rem(y, 2) * 2 + c
    )

    def send_heads(i, carry):
        tx = lax.rem(x + lax.div(i, 2), NX)
        ty = ty4 + 4 * lax.rem(i, 2)
        same = (tx == x) & (ty == y) & (tc4 == c)

        @pl.when(jnp.logical_not(same))
        def _():
            send(qs.at[lax.div(tx, 2)], qr.at[slot], 1, at(tx, ty, tc4))

        @pl.when(same)
        def _():
            qr[slot] = qs[lax.div(tx, 2)]

        return carry

    lax.fori_loop(0, 16, send_heads, 0)
    keeps_one = (lax.rem(y, 4) == ty4) & (tc4 == c)
    own_copy = pltpu.make_async_copy(arr.at[me], dec_mine, own_sem.at[0])
    own_copy.start()
    pages(0)

    @pl.when(keeps_one)
    def _():
        take(qr.at[pl.ds(0, 15)], rs.at[1])

    @pl.when(jnp.logical_not(keeps_one))
    def _():
        take(qr.at[pl.ds(0, 16)], rs.at[1])

    copies[9].wait()

    qf[...] = qr[...].astype(F32)

    rows8 = lax.broadcasted_iota(jnp.int32, (8, TILE), 0)
    rows16 = lax.broadcasted_iota(jnp.int32, (16, TILE), 0)
    scale = (D / HEADS) ** (-0.5)
    message = jnp.zeros((16, TILE), F32)
    row0 = lax.rem(my_group, 4) * 2
    for e in range(2):
        cos, sin = cosines[e], sines[e]

        def head(i):
            low = jnp.broadcast_to(qf[2 * i, pl.ds(row0 + e, 1), :], (8, TILE))
            high = jnp.broadcast_to(qf[2 * i + 1, pl.ds(row0 + e, 1), :], (8, TILE))
            return jnp.where(lane < HEAD_DIM // 2, low, high)

        def turned(u):
            return (u * cos + pltpu.roll(u, HEAD_DIM // 2, 1) * sin).astype(BF16).astype(F32)

        q = [turned(head(i)) for i in range(4)]
        k = [turned(head(4 + a)) for a in range(2)]
        v = [head(6 + a) for a in range(2)]
        zero = jnp.zeros((8, TILE), F32)
        left = jnp.where(rows8 == 0, q[0], jnp.where(rows8 == 1, q[1], zero))
        right = jnp.where(rows8 == 2, q[2], jnp.where(rows8 == 3, q[3], zero))
        own_raw = jnp.sum(left * k[0] + right * k[1], axis=1, keepdims=True) * scale
        own = jnp.exp(capped(own_raw))
        both = jnp.concatenate([left, right], axis=1).astype(BF16)
        raw = dot_t(both, cache[0, e]) * scale
        weights = jnp.where(seen[e], jnp.exp(capped(raw)), 0.0)
        den = jnp.sum(weights, axis=1, keepdims=True) + own
        num = dot_n(weights.astype(BF16), cache[1, e])
        own_b = own.astype(BF16).astype(F32)
        out_l = (num[:, :TILE] + own_b * v[0]) / den
        out_r = (num[:, TILE:] + own_b * v[1]) / den
        rows = [out_l[0:1], out_l[1:2], out_r[2:3], out_r[3:4], k[0][0:1], k[1][0:1], v[0][0:1], v[1][0:1]]
        for j, row in enumerate(rows):
            message = jnp.where(rows16 == e * 8 + j, jnp.broadcast_to(row, (16, TILE)), message)
    att_buf[c, x2, xp, y2, yp] = message.astype(BF16)

    first_leg(att_buf, 2)
    pages(1)
    second_leg(att_buf, 2)
    pages(2)
    last_leg(att_buf, 2)

    want = lax.broadcasted_iota(jnp.int32, (128, 256), 0)
    have = lax.broadcasted_iota(jnp.int32, (128, 256), 1)
    target = 8 * lax.rem(want, 32) + lax.div(want, 32)
    pick_q = jnp.where(have == target, 1.0, 0.0).astype(BF16)
    pick_kv = jnp.where(have == target + 4, 1.0, 0.0).astype(BF16)

    def by_slot(k):
        blocks = []
        for g in range(16):
            ay = (g % 2) * 4 + k // 2
            blocks.append(att_buf[k % 2, g // 4, (g // 2) % 2, ay // 2, ay % 2])
        return jnp.concatenate(blocks, axis=0)

    for k in range(PREFILL_TP):
        picked = dot_n(pick_q, by_slot(k)).astype(BF16)
        for h in range(4):
            att[:, pl.ds((4 * k + h) * TILE, TILE)] = picked[32 * h : 32 * h + 32]
    copies[6].wait()
    mixed_part = dot_t(att[...], wo[...]).astype(BF16)
    shift = lax.rem(me * COLS, TILE)
    src_col = lax.broadcasted_iota(jnp.int32, (COLS, TILE), 0)
    dst_col = lax.broadcasted_iota(jnp.int32, (COLS, TILE), 1)
    put0 = jnp.where(dst_col == lax.rem(src_col + shift, TILE), 1.0, 0.0).astype(BF16)
    put1 = jnp.where(dst_col == lax.rem(src_col + shift + 64, TILE), 1.0, 0.0).astype(BF16)
    mix_buf[c, x2, xp, y2, yp] = (dot_n(mixed_part[:16], put0) + dot_n(mixed_part[16:], put1)).astype(BF16)

    first_leg(mix_buf, 5)
    pages(3)
    for k in range(PREFILL_TP):
        picked = dot_n(pick_kv, by_slot(k)).astype(BF16)
        for a in range(2):
            nk_ref[:, pl.ds((2 * k + a) * TILE, TILE)] = picked[32 * a : 32 * a + 32]
            nv_ref[:, pl.ds((2 * k + a) * TILE, TILE)] = picked[64 + 32 * a : 96 + 32 * a]
    second_leg(mix_buf, 5)
    pages(4)
    last_leg(mix_buf, 5)

    lane16 = lax.broadcasted_iota(jnp.int32, (16, TILE), 1)

    def join(p, carry):
        straight, turned = [], []
        for i in range(32):
            piece = mix_buf[i % 2, p, i // 16, (i % 16) // 4, (i // 2) % 2].astype(F32)
            straight.append(piece)
            turned.append(pltpu.roll(piece, 64, 1))
        for t in range(9):
            top = bottom = None
            for i in range(32):
                lo, hi = COLS * i - TILE * t, COLS * i + COLS - TILE * t
                if hi <= 0 or lo >= TILE:
                    continue
                if top is None:
                    top, bottom = straight[i], turned[i]
                else:
                    later = lane16 >= lo
                    top = jnp.where(later, straight[i], top)
                    bottom = jnp.where(later, turned[i], bottom)
            column = pl.multiple_of((p * 9 + t) * TILE, TILE)
            mix[0:16, pl.ds(column, TILE)] = top
            mix[16:32, pl.ds(column, TILE)] = bottom
        return carry

    lax.fori_loop(0, 4, join, 0)
    stream[...] = hid[...] + rms_scale(mix[...], gain[1:2, :])
    ffn_in = rms_scale(stream[...], gain[2:3, :]).astype(BF16)
    copies[7].wait()
    gate = dot_t(ffn_in, wg[0])
    up = dot_t(ffn_in, wg[1])
    cube = gate + 0.044715 * (gate * gate * gate)
    active = (0.5 * gate * (1.0 + jnp.tanh(0.7978845608028654 * cube)) * up).astype(BF16)
    copies[8].wait()
    for n in range(4):
        columns = pl.ds(n * (D // 4), D // 4)
        piece = dot_n(active, wd[:, columns]).astype(BF16)
        br[0, :, columns] = piece[:16]
        br[1, :, columns] = piece[16:]

    send(br.at[1 - c], pr, 8, at(x, y, 1 - c))
    take(pr, rs.at[8])
    sb[...] = (br[c].astype(F32) + pr[...].astype(F32)).astype(BF16)

    def send_sums(j, carry):
        owner = lax.div(j * 16, 9)
        tile = sb.at[:, pl.ds(pl.multiple_of(j * TILE, TILE), TILE)]

        @pl.when(owner != chip)
        def _():
            send(tile, rs_buf.at[chip], 9, at(lax.div(owner, NY), lax.rem(owner, NY), c))

        @pl.when(owner == chip)
        def _():
            rs_buf[chip] = tile[...]

        return carry

    lax.fori_loop(0, TILES, send_sums, 0)
    pages(5)
    my_tile = lax.div(chip * 9 + 15, 16)
    owns = lax.div(my_tile * 16, 9) == chip

    @pl.when(owns)
    def _():
        take(rs_buf.at[pl.ds(0, CHIPS - 1)], rs.at[9])
        total = jnp.zeros((16, TILE), F32)

        def add(i, acc):
            for n in range(8):
                acc = acc + rs_buf[i * 8 + n].astype(F32)
            return acc

        fin[c, my_tile] = lax.fori_loop(0, 8, add, total).astype(BF16)

        def tell(i, carry):
            tx, ty = other_chip(i)
            send(fin.at[c, my_tile], fin.at[c, my_tile], 10, at(tx, ty, c))
            return carry

        lax.fori_loop(0, CHIPS - 1, tell, 0)

    pages(6)

    @pl.when(owns)
    def _():
        take(fin.at[0, pl.ds(0, TILES - 1)], rs.at[10])

    @pl.when(jnp.logical_not(owns))
    def _():
        take(fin.at[0, pl.ds(0, TILES)], rs.at[10])

    swap(fin, 11)
    take(fin.at[0], rs.at[11])

    first = lax.div(me * COLS, TILE)
    second = jnp.minimum(first + 1, TILES - 1)
    for half in range(2):

        def square(j, acc):
            for n in range(4):
                tile = fin[half, j * 4 + n].astype(F32)
                acc = acc + tile * tile
            return acc

        squares = lax.fori_loop(0, TILES // 4, square, jnp.zeros((16, TILE), F32))
        factor = lax.rsqrt(jnp.sum(squares, axis=1, keepdims=True) / D + EPSILON)

        def block(t):
            columns = pl.ds(pl.multiple_of(t * TILE, TILE), TILE)
            branch = fin[half, t].astype(F32)
            value = stream[16 * half : 16 * half + 16, columns] + branch * factor * (1.0 + gain[3:4, columns])
            return pltpu.roll(value, lax.rem(TILE - shift, TILE), 1)

        res_ref[16 * half : 16 * half + 16, :] = jnp.where(lane16 < TILE - shift, block(first), block(second))

    own_copy.wait()
    take(arr.at[pl.ds(0, GROUP - 1)], rs.at[0])
    take(arr.at[pl.ds(0, GROUP - 1)], ss.at[0])

    @pl.when(keeps_one)
    def _():
        take(qr.at[pl.ds(0, 15)], ss.at[1])

    @pl.when(jnp.logical_not(keeps_one))
    def _():
        take(qr.at[pl.ds(0, 16)], ss.at[1])

    gone(att_buf, 2)
    gone(mix_buf, 5)
    take(pr, ss.at[8])

    @pl.when(owns)
    def _():
        take(fin.at[0, pl.ds(0, TILES - 1)], ss.at[9])
        take(rs_buf.at[pl.ds(0, CHIPS - 1)], ss.at[10])

    @pl.when(jnp.logical_not(owns))
    def _():
        take(fin.at[0, pl.ds(0, TILES)], ss.at[9])

    take(fin.at[0], ss.at[11])


def on_device(
    hidden_in,
    prefill_cache,
    lengths,
    page_table,
    qkv_weight,
    out_weight,
    gate_up_weight,
    down_weight,
    norm_gains,
):
    me = lax.axis_index(TP)
    batch = hidden_in.shape[0]
    page_width = prefill_cache.shape[5]
    exponent = np.arange(HEAD_DIM // 2, dtype=np.float32) * np.float32(-2.0 / HEAD_DIM)
    frequency = np.power(np.float32(10000.0), exponent).astype(np.float32)
    frequency = jnp.asarray(np.concatenate([frequency, frequency])[None, :])
    paged = prefill_cache.reshape(2, 2, GROUP, page_width, 2 * HEAD_DIM)
    cache = prefill_cache.reshape(2, 2, GROUP * page_width, 2 * HEAD_DIM)
    k_cols = KV_HEADS * HEAD_DIM
    vmem = pl.BlockSpec(memory_space=pltpu.VMEM)
    hbm = pl.BlockSpec(memory_space=pltpu.HBM)
    dma = pltpu.SemaphoreType.DMA
    res, new_key, new_value, decoded = pl.pallas_call(
        step_kernel,
        name="step",
        out_shape=(
            jax.ShapeDtypeStruct((batch, TILE), F32),
            jax.ShapeDtypeStruct((batch, k_cols), BF16),
            jax.ShapeDtypeStruct((batch, k_cols), BF16),
            jax.ShapeDtypeStruct((1, 1, 2, batch, page_width, k_cols), BF16),
        ),
        in_specs=[pl.BlockSpec(memory_space=pltpu.SMEM)] + [hbm] * 10,
        out_specs=(vmem, vmem, vmem, pl.BlockSpec(memory_space=pl.ANY)),
        scratch_shapes=[
            pltpu.VMEM(page_table.shape, jnp.int32),
            pltpu.VMEM(frequency.shape, F32),
            pltpu.VMEM((16, GROUP), jnp.int32),
            pltpu.SMEM((16, GROUP), jnp.int32),
            pltpu.VMEM((batch, D), F32),
            pltpu.VMEM(paged.shape, BF16),
            pltpu.VMEM(cache.shape, BF16),
            pltpu.VMEM(qkv_weight.shape[1:], BF16),
            pltpu.VMEM(out_weight.shape[1:], BF16),
            pltpu.VMEM(gate_up_weight.shape[1:], BF16),
            pltpu.VMEM(down_weight.shape[1:], BF16),
            pltpu.VMEM(norm_gains.shape[1:], F32),
            pltpu.VMEM((GROUP, 2, 2, page_width, 2 * HEAD_DIM), BF16),
            pltpu.VMEM((4, 8, TILE), BF16),
            pltpu.VMEM((16, 8, TILE), BF16),
            pltpu.VMEM((16, 8, TILE), F32),
            pltpu.VMEM((NC, NX // 2, 2, NY // 2, 2, 16, TILE), BF16),
            pltpu.VMEM((batch, HEADS * HEAD_DIM), BF16),
            pltpu.VMEM((NC, NX // 2, 2, NY // 2, 2, 16, TILE), BF16),
            pltpu.VMEM((batch, D), F32),
            pltpu.VMEM((batch, D), F32),
            pltpu.VMEM((2, 16, D), BF16),
            pltpu.VMEM((16, D), BF16),
            pltpu.VMEM((16, D), BF16),
            pltpu.VMEM((CHIPS, 16, TILE), BF16),
            pltpu.VMEM((NC, TILES, 16, TILE), BF16),
            dma((10,)),
            dma((2,)),
            dma((12,)),
            dma((12,)),
        ],
        compiler_params=pltpu.CompilerParams(
            collective_id=0, has_side_effects=True, vmem_limit_bytes=48 * 2**20
        ),
    )(
        *[
            pltpu.with_memory_space_constraint(operand, pltpu.HBM)
            for operand in (
                lengths, page_table, frequency, hidden_in, paged, cache,
                qkv_weight, out_weight, gate_up_weight, down_weight, norm_gains,
            )
        ]
    )
    my_pos = me * page_width + jnp.arange(page_width, dtype=jnp.int32)
    fresh = (my_pos[None, :] == lengths[:, None])[None, None, None, :, :, None]
    new = jnp.stack([new_key, new_value], axis=0).reshape(1, 1, 2, batch, 1, k_cols)
    decode_cache = jnp.where(fresh, new, decoded)
    return (res[:, :COLS], decode_cache)


def solution(mesh):
    torus = Mesh(mesh.devices.reshape(mesh.shape["grp"], NX, NY, NC), ("grp",) + TP)
    return jax.shard_map(
        on_device,
        mesh=torus,
        in_specs=(
            P("grp", None),
            P(TP, None, None, "grp", None, None, None),
            P("grp"),
            P("grp", None),
            P(None, TP, None),
            P(None, TP, None),
            P(None, None, TP, None),
            P(None, TP, None),
            P(),
        ),
        out_specs=(P("grp", TP), P(TP, None, None, "grp", None, None)),
        check_vma=False,
    )
```

```python
import jax
import jax.numpy as jnp
import numpy as np
from jax import lax
from jax.experimental import pallas as pl
from jax.experimental.pallas import tpu as pltpu
from jax.sharding import Mesh
from jax.sharding import PartitionSpec as P

D = 4608
HEADS = 32
KV_HEADS = 16
HEAD_DIM = 128
PREFILL_TP = 8
NX, NY, NC = 8, 8, 2
CHIPS = NX * NY
GROUP = CHIPS * NC
COLS = D // GROUP
TILE = 128
TILES = D // TILE
TP = ("tp_0", "tp_1", "tp_2")
MESH = pl.DeviceIdType.MESH
BF16 = jnp.bfloat16
F32 = jnp.float32

EPSILON = 1e-06
SOFTCAP = 50.0

PAGES = (24, 12, 18, 0, 12, 18, 0, 20, 23)


def capped(raw_scores):
    return SOFTCAP * jnp.tanh(raw_scores / SOFTCAP)


def rms_scale(vector, gain_row):
    meansq = jnp.mean(vector * vector, axis=-1, keepdims=True)
    return vector * lax.rsqrt(meansq + EPSILON) * (1.0 + gain_row)


def dot_t(left, right):
    return lax.dot_general(left, right, (((1,), (1,)), ((), ())), preferred_element_type=F32)


def dot_n(left, right):
    return jnp.dot(left, right, preferred_element_type=F32)


def step_kernel(
    len_ref, table_hbm, freq_hbm, hid_hbm, paged_hbm, cache_hbm, wq_hbm, wo_hbm, wg_hbm, wd_hbm, gain_hbm,
    res_ref, nk_ref, nv_ref, dec_ref,
    table, freq, inv_v, inv, hid, paged, cache, wq, wo, wg, wd, gain, arr, qs, qr, qf, att_buf, att, mix_buf, mix, stream,
    br, pr, sb, rs_buf, fin, sqs, marks, in_sem, own_sem, ss, rs,
):
    grp = lax.axis_index("grp")
    x = lax.axis_index("tp_0")
    y = lax.axis_index("tp_1")
    c = lax.axis_index("tp_2")
    chip = x * NY + y
    me = chip * NC + c
    my_group = lax.div(me, PREFILL_TP)
    my_slot = lax.rem(me, PREFILL_TP)

    def at(tx, ty, tc):
        return (grp, tx, ty, tc)

    barrier = pltpu.get_barrier_semaphore()

    def peer(i):
        tx = lax.rem(x + lax.div(i, NY * NC), NX)
        ty = lax.rem(y + lax.rem(lax.div(i, NC), NY), NY)
        tc = lax.rem(c + lax.rem(i, NC), NC)
        return tx, ty, tc

    def greet(i, carry):
        pl.semaphore_signal(barrier, inc=1, device_id=at(*peer(i)), device_id_type=MESH)
        return carry

    loads = [
        (table_hbm, table), (freq_hbm, freq), (hid_hbm, hid),
        (gain_hbm.at[0], gain), (wq_hbm.at[0], wq), (paged_hbm, paged),
        (wo_hbm.at[0], wo), (wg_hbm.at[0], wg), (wd_hbm.at[0], wd), (cache_hbm, cache),
    ]
    copies = [pltpu.make_async_copy(s, d, in_sem.at[n]) for n, (s, d) in enumerate(loads)]
    for copy in copies:
        copy.start()
    lax.fori_loop(1, GROUP, greet, 0)

    def send(src, dst, phase, target):
        pltpu.make_async_remote_copy(
            src_ref=src, dst_ref=dst, send_sem=ss.at[phase], recv_sem=rs.at[phase],
            device_id=target, device_id_type=MESH,
        ).start()

    def take(ref, sem):
        pltpu.make_async_copy(ref, ref, sem).wait()

    def each(first, last, width, body):
        whole = (last - first) // width

        def several(n, carry):
            for k in range(width):
                body(first + n * width + k)
            return carry

        if whole:
            lax.fori_loop(0, whole, several, 0)
        for n in range(first + whole * width, last):
            body(n)

    dec_mine = dec_ref.at[0, 0, :, pl.ds(my_group * 2, 2), :, pl.ds(pl.multiple_of(my_slot * 256, 256), 256)]

    def page_peer(j):
        tx, ty, tc = peer(lax.rem(j * 37, GROUP))
        return (tx * NY + ty) * NC + tc, at(tx, ty, tc)

    def send_page(j):
        number, target = page_peer(j)
        send(arr.at[number], dec_mine, 0, target)

    def arrange(j):
        number, _ = page_peer(j)
        for e in range(2):
            page = jnp.maximum(jnp.minimum(inv[8 * e, number], GROUP - 1), 0)
            for kv in range(2):
                arr[number, kv, e] = paged[kv, e, page]

    def pages(n):
        first = 1 + sum(PAGES[:n])
        each(first, first + PAGES[n], 4, send_page)

    def other_chip(i):
        n = i + lax.div(i, 36)
        tx = lax.rem(x + 4 + lax.div(n, NY), NX)
        ty = lax.rem(y + 4 + lax.rem(n, NY), NY)
        return tx, ty

    x2, xp, y2, yp = lax.div(x, 2), lax.rem(x, 2), lax.div(y, 2), lax.rem(y, 2)
    even = 1 - lax.rem(x + y, 2)

    def mine(buf):
        return buf.at[c, x2, xp, y2, yp]

    def first_leg(buf, phase):
        for o in (4, 3, 5, 2, 6, 1, 7):
            target = at(lax.rem(x + even * o, NX), lax.rem(y + (1 - even) * o, NY), c)
            send(mine(buf), mine(buf), phase, target)

    def second_leg(buf, phase):
        take(rs_buf.at[pl.ds(0, 7)], rs.at[phase])
        row = buf.at[c, :, yp, y2, yp]
        column = buf.at[c, x2, xp, :, 1 - xp]
        for o in (4, 3, 5, 2, 6, 1, 7):
            send(row, row, phase + 1, at(x, lax.rem(y + o, NY), c))
            send(column, column, phase + 1, at(lax.rem(x + o, NX), y, c))

    def last_leg(buf, phase, portion):
        take(rs_buf.at[pl.ds(0, 56)], rs.at[phase + 1])
        swap(buf, phase + 2)
        pages(portion)
        take(buf.at[0], rs.at[phase + 2])

    def gone(buf, phase):
        take(rs_buf.at[pl.ds(0, 7)], ss.at[phase])
        take(rs_buf.at[pl.ds(0, 56)], ss.at[phase + 1])
        take(buf.at[0], ss.at[phase + 2])

    def swap(buf, phase):
        send(buf.at[c], buf.at[c], phase, at(x, y, 1 - c))

    copies[2].wait()
    copies[3].wait()
    normed = rms_scale(hid[...], gain[0:1, :]).astype(BF16)
    copies[4].wait()
    part = dot_t(normed, wq[...]).astype(BF16)
    part = jnp.concatenate([part, part], axis=1)
    for t in range(4):
        qs[t] = part[8 * t : 8 * t + 8]

    copies[0].wait()
    block = lax.broadcasted_iota(jnp.int32, (GROUP, GROUP), 0)
    index = lax.broadcasted_iota(jnp.int32, (8, GROUP), 1).astype(F32).astype(BF16)
    tables = []
    for e in range(2):
        row = table[pl.ds(my_group * 2 + e, 1), :]
        tables.append(row)
        hits = jnp.where(jnp.broadcast_to(row, (GROUP, GROUP)) == block, 1.0, 0.0).astype(BF16)
        inv_v[8 * e : 8 * e + 8, :] = dot_t(index, hits).astype(jnp.int32)
    to_scalars = pltpu.make_async_copy(inv_v, inv, own_sem.at[1])
    to_scalars.start()

    copies[5].wait()
    to_scalars.wait()

    each(0, 1 + PAGES[0], 4, arrange)
    fin[...] = jnp.zeros(fin.shape, BF16)
    pl.semaphore_wait(barrier, GROUP - 1)

    is_kv = lax.div(x, 4)
    xx = lax.rem(x, 2)
    ty4 = (1 - is_kv) * x + is_kv * (xx * 2 + lax.div(y, 4))
    tc4 = (1 - is_kv) * lax.div(y, 4) + is_kv * lax.rem(lax.div(y, 2), 2)
    slot = (1 - is_kv) * (lax.rem(y, 4) * 2 + c) + is_kv * (
        8 + lax.div(lax.rem(x, 4), 2) * 4 + lax.rem(y, 2) * 2 + c
    )

    def send_heads(i, carry):
        tx = lax.rem(x + lax.div(i, 2), NX)
        ty = ty4 + 4 * lax.rem(i, 2)
        same = (tx == x) & (ty == y) & (tc4 == c)

        @pl.when(jnp.logical_not(same))
        def _():
            send(qs.at[lax.div(tx, 2)], qr.at[slot], 1, at(tx, ty, tc4))

        @pl.when(same)
        def _():
            qr[slot] = qs[lax.div(tx, 2)]

        return carry

    lax.fori_loop(0, 16, send_heads, 0)
    keeps_one = (lax.rem(y, 4) == ty4) & (tc4 == c)
    own_copy = pltpu.make_async_copy(arr.at[me], dec_mine, own_sem.at[0])
    own_copy.start()
    pages(0)
    each(1 + PAGES[0], GROUP, 4, arrange)

    copies[1].wait()
    slot_page = lax.broadcasted_iota(jnp.int32, (GROUP, GROUP * 8), 0)
    slot_at = lax.broadcasted_iota(jnp.int32, (GROUP, GROUP * 8), 1)
    widen = jnp.where(lax.div(slot_at, 8) == slot_page, 1.0, 0.0).astype(BF16)
    token = lax.rem(lax.broadcasted_iota(jnp.int32, (8, GROUP * 8), 1), 8).astype(F32)
    lane = lax.broadcasted_iota(jnp.int32, (8, TILE), 1)
    seen, cosines, sines = [], [], []
    for e in range(2):
        length = len_ref[my_group * 2 + e].astype(F32)
        row = jnp.broadcast_to(tables[e], (8, GROUP)).astype(F32).astype(BF16)
        seen.append(dot_n(row, widen) * 8.0 + token < length)
        angle = jnp.broadcast_to(freq[...], (8, TILE)) * length
        sine = jnp.sin(angle)
        cosines.append(jnp.cos(angle))
        sines.append(jnp.where(lane < HEAD_DIM // 2, -sine, sine))


    @pl.when(keeps_one)
    def _():
        take(qr.at[pl.ds(0, 15)], rs.at[1])

    @pl.when(jnp.logical_not(keeps_one))
    def _():
        take(qr.at[pl.ds(0, 16)], rs.at[1])

    copies[9].wait()

    qf[...] = qr[...].astype(F32)

    rows8 = lax.broadcasted_iota(jnp.int32, (8, TILE), 0)
    rows16 = lax.broadcasted_iota(jnp.int32, (16, TILE), 0)
    scale = (D / HEADS) ** (-0.5)
    message = jnp.zeros((16, TILE), F32)
    row0 = lax.rem(my_group, 4) * 2
    for e in range(2):
        cos, sin = cosines[e], sines[e]

        def head(i):
            low = jnp.broadcast_to(qf[2 * i, pl.ds(row0 + e, 1), :], (8, TILE))
            high = jnp.broadcast_to(qf[2 * i + 1, pl.ds(row0 + e, 1), :], (8, TILE))
            return jnp.where(lane < HEAD_DIM // 2, low, high)

        def turned(u):
            return (u * cos + pltpu.roll(u, HEAD_DIM // 2, 1) * sin).astype(BF16).astype(F32)

        q = [turned(head(i)) for i in range(4)]
        k = [turned(head(4 + a)) for a in range(2)]
        v = [head(6 + a) for a in range(2)]
        zero = jnp.zeros((8, TILE), F32)
        left = jnp.where(rows8 == 0, q[0], jnp.where(rows8 == 1, q[1], zero))
        right = jnp.where(rows8 == 2, q[2], jnp.where(rows8 == 3, q[3], zero))
        own_raw = jnp.sum(left * k[0] + right * k[1], axis=1, keepdims=True) * scale
        own = jnp.exp(capped(own_raw))
        both = jnp.concatenate([left, right], axis=1).astype(BF16)
        raw = dot_t(both, cache[0, e]) * scale
        weights = jnp.where(seen[e], jnp.exp(capped(raw)), 0.0)
        den = jnp.sum(weights, axis=1, keepdims=True) + own
        num = dot_n(weights.astype(BF16), cache[1, e])
        own_b = own.astype(BF16).astype(F32)
        out_l = (num[:, :TILE] + own_b * v[0]) / den
        out_r = (num[:, TILE:] + own_b * v[1]) / den
        rows = [out_l[0:1], out_l[1:2], out_r[2:3], out_r[3:4], k[0][0:1], k[1][0:1], v[0][0:1], v[1][0:1]]
        for j, row in enumerate(rows):
            message = jnp.where(rows16 == e * 8 + j, jnp.broadcast_to(row, (16, TILE)), message)
    att_buf[c, x2, xp, y2, yp] = message.astype(BF16)

    first_leg(att_buf, 2)
    pages(1)
    second_leg(att_buf, 2)
    pages(2)
    last_leg(att_buf, 2, 3)

    want = lax.broadcasted_iota(jnp.int32, (128, 256), 0)
    have = lax.broadcasted_iota(jnp.int32, (128, 256), 1)
    target = 8 * lax.rem(want, 32) + lax.div(want, 32)
    pick_q = jnp.where(have == target, 1.0, 0.0).astype(BF16)
    pick_kv = jnp.where(have == target + 4, 1.0, 0.0).astype(BF16)

    def by_slot(k):
        blocks = []
        for g in range(16):
            ay = (g % 2) * 4 + k // 2
            blocks.append(att_buf[k % 2, g // 4, (g // 2) % 2, ay // 2, ay % 2])
        return jnp.concatenate(blocks, axis=0)

    for k in range(PREFILL_TP):
        picked = dot_n(pick_q, by_slot(k)).astype(BF16)
        for h in range(4):
            att[:, pl.ds((4 * k + h) * TILE, TILE)] = picked[32 * h : 32 * h + 32]
    copies[6].wait()
    mixed_part = dot_t(att[...], wo[...]).astype(BF16)
    shift = lax.rem(me * COLS, TILE)
    src_col = lax.broadcasted_iota(jnp.int32, (COLS, TILE), 0)
    dst_col = lax.broadcasted_iota(jnp.int32, (COLS, TILE), 1)
    put0 = jnp.where(dst_col == lax.rem(src_col + shift, TILE), 1.0, 0.0).astype(BF16)
    put1 = jnp.where(dst_col == lax.rem(src_col + shift + 64, TILE), 1.0, 0.0).astype(BF16)
    mix_buf[c, x2, xp, y2, yp] = (dot_n(mixed_part[:16], put0) + dot_n(mixed_part[16:], put1)).astype(BF16)

    first_leg(mix_buf, 5)
    pages(4)
    for k in range(PREFILL_TP):
        picked = dot_n(pick_kv, by_slot(k)).astype(BF16)
        for a in range(2):
            nk_ref[:, pl.ds((2 * k + a) * TILE, TILE)] = picked[32 * a : 32 * a + 32]
            nv_ref[:, pl.ds((2 * k + a) * TILE, TILE)] = picked[64 + 32 * a : 96 + 32 * a]
    second_leg(mix_buf, 5)
    pages(5)
    last_leg(mix_buf, 5, 6)

    lane16 = lax.broadcasted_iota(jnp.int32, (16, TILE), 1)

    def join(p, carry):
        straight, turned = [], []
        for i in range(32):
            piece = mix_buf[i % 2, p, i // 16, (i % 16) // 4, (i // 2) % 2].astype(F32)
            straight.append(piece)
            turned.append(pltpu.roll(piece, 64, 1))
        for t in range(9):
            top = bottom = None
            for i in range(32):
                lo, hi = COLS * i - TILE * t, COLS * i + COLS - TILE * t
                if hi <= 0 or lo >= TILE:
                    continue
                if top is None:
                    top, bottom = straight[i], turned[i]
                else:
                    later = lane16 >= lo
                    top = jnp.where(later, straight[i], top)
                    bottom = jnp.where(later, turned[i], bottom)
            column = pl.multiple_of((p * 9 + t) * TILE, TILE)
            mix[0:16, pl.ds(column, TILE)] = top
            mix[16:32, pl.ds(column, TILE)] = bottom
        return carry

    lax.fori_loop(0, 4, join, 0)
    stream[...] = hid[...] + rms_scale(mix[...], gain[1:2, :])
    ffn_in = rms_scale(stream[...], gain[2:3, :]).astype(BF16)
    copies[7].wait()
    gate = dot_t(ffn_in, wg[0])
    up = dot_t(ffn_in, wg[1])
    cube = gate + 0.044715 * (gate * gate * gate)
    active = (0.5 * gate * (1.0 + jnp.tanh(0.7978845608028654 * cube)) * up).astype(BF16)
    copies[8].wait()
    for n in range(4):
        columns = pl.ds(n * (D // 4), D // 4)
        piece = dot_n(active, wd[:, columns]).astype(BF16)
        br[0, :, columns] = piece[:16]
        br[1, :, columns] = piece[16:]

    send(br.at[1 - c], pr, 8, at(x, y, 1 - c))
    take(pr, rs.at[8])
    sb[...] = (br[c].astype(F32) + pr[...].astype(F32)).astype(BF16)

    def send_sums(j):
        owner = lax.div(j * 16, 9)
        tile = sb.at[:, pl.ds(pl.multiple_of(j * TILE, TILE), TILE)]

        @pl.when(owner != chip)
        def _():
            send(tile, rs_buf.at[chip], 9, at(lax.div(owner, NY), lax.rem(owner, NY), c))

        @pl.when(owner == chip)
        def _():
            rs_buf[chip] = tile[...]

    each(0, TILES, 6, send_sums)
    pages(7)
    my_tile = lax.div(chip * 9 + 15, 16)
    owns = lax.div(my_tile * 16, 9) == chip
    chip_cols = NC * COLS
    last_reader = lax.div(my_tile * TILE + TILE - 1, chip_cols)
    low = lax.div(chip * chip_cols, TILE)
    high = lax.div(chip * chip_cols + chip_cols - 1, TILE)
    low_tile = jnp.minimum(low, TILES - 2)
    needs_low = lax.div(low * 16, 9) != chip
    needs_high = (high != low) & (lax.div(high * 16, 9) != chip)

    @pl.when(owns)
    def _():
        take(rs_buf.at[pl.ds(0, CHIPS - 1)], rs.at[9])
        total = jnp.zeros((16, TILE), F32)

        def add(i, acc):
            for n in range(8):
                acc = acc + rs_buf[i * 8 + n].astype(F32)
            return acc

        total = lax.fori_loop(0, 8, add, total)
        fin[c, my_tile] = total.astype(BF16)
        squares = jnp.sum(total * total, axis=1, keepdims=True)
        sqs[c, my_tile] = jnp.sum(jnp.where(rows16 == lane16, squares, 0.0), axis=0, keepdims=True)
        for ahead in (1, 2):

            @pl.when(chip + ahead <= last_reader)
            def _():
                reader = chip + ahead
                send(fin.at[c, my_tile], fin.at[c, my_tile], 12, at(lax.div(reader, NY), lax.rem(reader, NY), c))

        def tell(i):
            tx, ty = other_chip(i)
            send(sqs.at[c, my_tile], sqs.at[c, my_tile], 10, at(tx, ty, c))

        each(0, CHIPS - 1, 9, tell)

    pages(8)

    @pl.when(owns)
    def _():
        take(sqs.at[0, pl.ds(0, TILES - 1)], rs.at[10])

    @pl.when(jnp.logical_not(owns))
    def _():
        take(sqs.at[0, pl.ds(0, TILES)], rs.at[10])

    @pl.when(needs_low & needs_high)
    def _():
        take(fin.at[0, pl.ds(0, 2)], rs.at[12])

    @pl.when(needs_low != needs_high)
    def _():
        take(fin.at[0, pl.ds(0, 1)], rs.at[12])

    swap(sqs, 11)
    send(fin.at[c, pl.ds(low_tile, 2)], fin.at[c, pl.ds(low_tile, 2)], 13, at(x, y, 1 - c))
    take(sqs.at[0], rs.at[11])
    take(fin.at[0, pl.ds(0, 2)], rs.at[13])

    first = lax.div(me * COLS, TILE)
    second = jnp.minimum(first + 1, TILES - 1)
    for half in range(2):

        squares = jnp.zeros((1, TILE), F32)
        for t in range(TILES):
            squares = squares + sqs[half, t]
        by_row = jnp.where(rows16 == lane16, jnp.broadcast_to(squares, (16, TILE)), 0.0)
        factor = lax.rsqrt(jnp.sum(by_row, axis=1, keepdims=True) / D + EPSILON)

        def block(t):
            columns = pl.ds(pl.multiple_of(t * TILE, TILE), TILE)
            branch = fin[half, t].astype(F32)
            value = stream[16 * half : 16 * half + 16, columns] + branch * factor * (1.0 + gain[3:4, columns])
            return pltpu.roll(value, lax.rem(TILE - shift, TILE), 1)

        res_ref[16 * half : 16 * half + 16, :] = jnp.where(lane16 < TILE - shift, block(first), block(second))

    own_copy.wait()
    take(arr.at[pl.ds(0, GROUP - 1)], rs.at[0])
    take(arr.at[pl.ds(0, GROUP - 1)], ss.at[0])

    @pl.when(keeps_one)
    def _():
        take(qr.at[pl.ds(0, 15)], ss.at[1])

    @pl.when(jnp.logical_not(keeps_one))
    def _():
        take(qr.at[pl.ds(0, 16)], ss.at[1])

    gone(att_buf, 2)
    gone(mix_buf, 5)
    take(pr, ss.at[8])

    @pl.when(owns)
    def _():
        take(fin.at[0, pl.ds(0, TILES - 1)], ss.at[9])
        take(marks, ss.at[10])

        @pl.when(chip + 2 <= last_reader)
        def _():
            take(fin.at[0, pl.ds(0, 2)], ss.at[12])

        @pl.when((chip + 1 <= last_reader) & (chip + 2 > last_reader))
        def _():
            take(fin.at[0, pl.ds(0, 1)], ss.at[12])

    @pl.when(jnp.logical_not(owns))
    def _():
        take(fin.at[0, pl.ds(0, TILES)], ss.at[9])

    take(sqs.at[0], ss.at[11])
    take(fin.at[0, pl.ds(0, 2)], ss.at[13])


def on_device(
    hidden_in,
    prefill_cache,
    lengths,
    page_table,
    qkv_weight,
    out_weight,
    gate_up_weight,
    down_weight,
    norm_gains,
):
    me = lax.axis_index(TP)
    batch = hidden_in.shape[0]
    page_width = prefill_cache.shape[5]
    exponent = np.arange(HEAD_DIM // 2, dtype=np.float32) * np.float32(-2.0 / HEAD_DIM)
    frequency = np.power(np.float32(10000.0), exponent).astype(np.float32)
    frequency = jnp.asarray(np.concatenate([frequency, frequency])[None, :])
    paged = prefill_cache.reshape(2, 2, GROUP, page_width, 2 * HEAD_DIM)
    cache = prefill_cache.reshape(2, 2, GROUP * page_width, 2 * HEAD_DIM)
    k_cols = KV_HEADS * HEAD_DIM
    vmem = pl.BlockSpec(memory_space=pltpu.VMEM)
    hbm = pl.BlockSpec(memory_space=pltpu.HBM)
    dma = pltpu.SemaphoreType.DMA
    res, new_key, new_value, decoded = pl.pallas_call(
        step_kernel,
        name="step",
        out_shape=(
            jax.ShapeDtypeStruct((batch, TILE), F32),
            jax.ShapeDtypeStruct((batch, k_cols), BF16),
            jax.ShapeDtypeStruct((batch, k_cols), BF16),
            jax.ShapeDtypeStruct((1, 1, 2, batch, page_width, k_cols), BF16),
        ),
        in_specs=[pl.BlockSpec(memory_space=pltpu.SMEM)] + [hbm] * 10,
        out_specs=(vmem, vmem, vmem, pl.BlockSpec(memory_space=pl.ANY)),
        scratch_shapes=[
            pltpu.VMEM(page_table.shape, jnp.int32),
            pltpu.VMEM(frequency.shape, F32),
            pltpu.VMEM((16, GROUP), jnp.int32),
            pltpu.SMEM((16, GROUP), jnp.int32),
            pltpu.VMEM((batch, D), F32),
            pltpu.VMEM(paged.shape, BF16),
            pltpu.VMEM(cache.shape, BF16),
            pltpu.VMEM(qkv_weight.shape[1:], BF16),
            pltpu.VMEM(out_weight.shape[1:], BF16),
            pltpu.VMEM(gate_up_weight.shape[1:], BF16),
            pltpu.VMEM(down_weight.shape[1:], BF16),
            pltpu.VMEM(norm_gains.shape[1:], F32),
            pltpu.VMEM((GROUP, 2, 2, page_width, 2 * HEAD_DIM), BF16),
            pltpu.VMEM((4, 8, TILE), BF16),
            pltpu.VMEM((16, 8, TILE), BF16),
            pltpu.VMEM((16, 8, TILE), F32),
            pltpu.VMEM((NC, NX // 2, 2, NY // 2, 2, 16, TILE), BF16),
            pltpu.VMEM((batch, HEADS * HEAD_DIM), BF16),
            pltpu.VMEM((NC, NX // 2, 2, NY // 2, 2, 16, TILE), BF16),
            pltpu.VMEM((batch, D), F32),
            pltpu.VMEM((batch, D), F32),
            pltpu.VMEM((2, 16, D), BF16),
            pltpu.VMEM((16, D), BF16),
            pltpu.VMEM((16, D), BF16),
            pltpu.VMEM((CHIPS, 16, TILE), BF16),
            pltpu.VMEM((NC, TILES, 16, TILE), BF16),
            pltpu.VMEM((NC, TILES, 1, TILE), F32),
            pltpu.VMEM((CHIPS - 1, 1, TILE), F32),
            dma((10,)),
            dma((2,)),
            dma((14,)),
            dma((14,)),
        ],
        compiler_params=pltpu.CompilerParams(
            collective_id=0, has_side_effects=True, vmem_limit_bytes=48 * 2**20
        ),
    )(
        *[
            pltpu.with_memory_space_constraint(operand, pltpu.HBM)
            for operand in (
                lengths, page_table, frequency, hidden_in, paged, cache,
                qkv_weight, out_weight, gate_up_weight, down_weight, norm_gains,
            )
        ]
    )
    my_pos = me * page_width + jnp.arange(page_width, dtype=jnp.int32)
    fresh = (my_pos[None, :] == lengths[:, None])[None, None, None, :, :, None]
    new = jnp.stack([new_key, new_value], axis=0).reshape(1, 1, 2, batch, 1, k_cols)
    decode_cache = jnp.where(fresh, new, decoded)
    return (res[:, :COLS], decode_cache)


def solution(mesh):
    torus = Mesh(mesh.devices.reshape(mesh.shape["grp"], NX, NY, NC), ("grp",) + TP)
    return jax.shard_map(
        on_device,
        mesh=torus,
        in_specs=(
            P("grp", None),
            P(TP, None, None, "grp", None, None, None),
            P("grp"),
            P("grp", None),
            P(None, TP, None),
            P(None, TP, None),
            P(None, None, TP, None),
            P(None, TP, None),
            P(),
        ),
        out_specs=(P("grp", TP), P(TP, None, None, "grp", None, None)),
        check_vma=False,
    )
```

```python
import jax
import jax.numpy as jnp
import numpy as np
from jax import lax
from jax.experimental import pallas as pl
from jax.experimental.pallas import tpu as pltpu
from jax.sharding import Mesh
from jax.sharding import PartitionSpec as P

D = 4608
HEADS = 32
KV_HEADS = 16
HEAD_DIM = 128
PREFILL_TP = 8
NX, NY, NC = 8, 8, 2
CHIPS = NX * NY
GROUP = CHIPS * NC
COLS = D // GROUP
TILE = 128
TILES = D // TILE
TP = ("tp_0", "tp_1", "tp_2")
MESH = pl.DeviceIdType.MESH
BF16 = jnp.bfloat16
F32 = jnp.float32

EPSILON = 1e-06
SOFTCAP = 50.0

PAGES = (24, 12, 18, 0, 12, 18, 0, 20, 23)


def capped(raw_scores):
    return SOFTCAP * jnp.tanh(raw_scores / SOFTCAP)


def rms_scale(vector, gain_row):
    meansq = jnp.mean(vector * vector, axis=-1, keepdims=True)
    return vector * lax.rsqrt(meansq + EPSILON) * (1.0 + gain_row)


def dot_t(left, right):
    return lax.dot_general(left, right, (((1,), (1,)), ((), ())), preferred_element_type=F32)


def dot_n(left, right):
    return jnp.dot(left, right, preferred_element_type=F32)


def step_kernel(
    len_ref, table_hbm, freq_hbm, hid_hbm, paged_hbm, cache_hbm, wq_hbm, wo_hbm, wg_hbm, wd_hbm, gain_hbm,
    res_ref, nk_ref, nv_ref, fresh_ref, dec_ref,
    table, freq, inv_v, inv, hid, paged, cache, wq, wo, wg, wd, gain, arr, qs, qr, qf, att_buf, att, mix_buf, mix, stream,
    br, pr, sb, rs_buf, fin, sqs, marks, in_sem, own_sem, ss, rs,
):
    grp = lax.axis_index("grp")
    x = lax.axis_index("tp_0")
    y = lax.axis_index("tp_1")
    c = lax.axis_index("tp_2")
    chip = x * NY + y
    me = chip * NC + c
    my_group = lax.div(me, PREFILL_TP)
    my_slot = lax.rem(me, PREFILL_TP)

    def at(tx, ty, tc):
        return (grp, tx, ty, tc)

    barrier = pltpu.get_barrier_semaphore()

    def peer(i):
        tx = lax.rem(x + lax.div(i, NY * NC), NX)
        ty = lax.rem(y + lax.rem(lax.div(i, NC), NY), NY)
        tc = lax.rem(c + lax.rem(i, NC), NC)
        return tx, ty, tc

    def greet(i, carry):
        pl.semaphore_signal(barrier, inc=1, device_id=at(*peer(i)), device_id_type=MESH)
        return carry

    loads = [
        (table_hbm, table), (freq_hbm, freq), (hid_hbm, hid),
        (gain_hbm.at[0], gain), (wq_hbm.at[0], wq), (paged_hbm, paged),
        (wo_hbm.at[0], wo), (wg_hbm.at[0], wg), (wd_hbm.at[0], wd), (cache_hbm, cache),
    ]
    copies = [pltpu.make_async_copy(s, d, in_sem.at[n]) for n, (s, d) in enumerate(loads)]
    for copy in copies:
        copy.start()
    lax.fori_loop(1, GROUP, greet, 0)

    def send(src, dst, phase, target):
        pltpu.make_async_remote_copy(
            src_ref=src, dst_ref=dst, send_sem=ss.at[phase], recv_sem=rs.at[phase],
            device_id=target, device_id_type=MESH,
        ).start()

    def take(ref, sem):
        pltpu.make_async_copy(ref, ref, sem).wait()

    def each(first, last, width, body):
        whole = (last - first) // width

        def several(n, carry):
            for k in range(width):
                body(first + n * width + k)
            return carry

        if whole:
            lax.fori_loop(0, whole, several, 0)
        for n in range(first + whole * width, last):
            body(n)

    dec_mine = dec_ref.at[0, 0, :, pl.ds(my_group * 2, 2), :, pl.ds(pl.multiple_of(my_slot * 256, 256), 256)]

    def page_peer(j):
        tx, ty, tc = peer(lax.rem(j * 53, GROUP))
        return (tx * NY + ty) * NC + tc, at(tx, ty, tc)

    def send_page(j):
        number, target = page_peer(j)
        send(arr.at[number], dec_mine, 0, target)

    def arrange(j):
        number, _ = page_peer(j)
        for e in range(2):
            page = jnp.maximum(jnp.minimum(inv[8 * e, number], GROUP - 1), 0)
            for kv in range(2):
                arr[number, kv, e] = paged[kv, e, page]

    def pages(n):
        first = 1 + sum(PAGES[:n])
        each(first, first + PAGES[n], 4, send_page)

    def other_chip(i):
        n = i + lax.div(i, 36)
        tx = lax.rem(x + 4 + lax.div(n, NY), NX)
        ty = lax.rem(y + 4 + lax.rem(n, NY), NY)
        return tx, ty

    x2, xp, y2, yp = lax.div(x, 2), lax.rem(x, 2), lax.div(y, 2), lax.rem(y, 2)
    even = 1 - lax.rem(x + y, 2)

    def mine(buf):
        return buf.at[c, x2, xp, y2, yp]

    def first_leg(buf, phase):
        for o in (4, 3, 5, 2, 6, 1, 7):
            target = at(lax.rem(x + even * o, NX), lax.rem(y + (1 - even) * o, NY), c)
            send(mine(buf), mine(buf), phase, target)

    def second_leg(buf, phase):
        take(rs_buf.at[pl.ds(0, 7)], rs.at[phase])
        row = buf.at[c, :, yp, y2, yp]
        column = buf.at[c, x2, xp, :, 1 - xp]
        for o in (4, 3, 5, 2, 6, 1, 7):
            send(row, row, phase + 1, at(x, lax.rem(y + o, NY), c))
            send(column, column, phase + 1, at(lax.rem(x + o, NX), y, c))

    def last_leg(buf, phase, portion):
        take(rs_buf.at[pl.ds(0, 56)], rs.at[phase + 1])
        swap(buf, phase + 2)
        pages(portion)
        take(buf.at[0], rs.at[phase + 2])

    def gone(buf, phase):
        take(rs_buf.at[pl.ds(0, 7)], ss.at[phase])
        take(rs_buf.at[pl.ds(0, 56)], ss.at[phase + 1])
        take(buf.at[0], ss.at[phase + 2])

    def swap(buf, phase):
        send(buf.at[c], buf.at[c], phase, at(x, y, 1 - c))

    copies[2].wait()
    copies[3].wait()
    normed = rms_scale(hid[...], gain[0:1, :]).astype(BF16)
    copies[4].wait()
    part = dot_t(normed, wq[...]).astype(BF16)
    part = jnp.concatenate([part, part], axis=1)
    for t in range(4):
        qs[t] = part[8 * t : 8 * t + 8]

    copies[0].wait()
    block = lax.broadcasted_iota(jnp.int32, (GROUP, GROUP), 0)
    index = lax.broadcasted_iota(jnp.int32, (8, GROUP), 1).astype(F32).astype(BF16)
    tables = []
    for e in range(2):
        row = table[pl.ds(my_group * 2 + e, 1), :]
        tables.append(row)
        hits = jnp.where(jnp.broadcast_to(row, (GROUP, GROUP)) == block, 1.0, 0.0).astype(BF16)
        inv_v[8 * e : 8 * e + 8, :] = dot_t(index, hits).astype(jnp.int32)
    to_scalars = pltpu.make_async_copy(inv_v, inv, own_sem.at[1])
    to_scalars.start()

    copies[5].wait()
    to_scalars.wait()

    each(0, 1 + PAGES[0], 4, arrange)
    fin[...] = jnp.zeros(fin.shape, BF16)
    pl.semaphore_wait(barrier, GROUP - 1)

    is_kv = lax.div(x, 4)
    xx = lax.rem(x, 2)
    ty4 = (1 - is_kv) * x + is_kv * (xx * 2 + lax.div(y, 4))
    tc4 = (1 - is_kv) * lax.div(y, 4) + is_kv * lax.rem(lax.div(y, 2), 2)
    slot = (1 - is_kv) * (lax.rem(y, 4) * 2 + c) + is_kv * (
        8 + lax.div(lax.rem(x, 4), 2) * 4 + lax.rem(y, 2) * 2 + c
    )

    def send_heads(i, carry):
        tx = lax.rem(x + lax.div(i, 2), NX)
        ty = ty4 + 4 * lax.rem(i, 2)
        same = (tx == x) & (ty == y) & (tc4 == c)

        @pl.when(jnp.logical_not(same))
        def _():
            send(qs.at[lax.div(tx, 2)], qr.at[slot], 1, at(tx, ty, tc4))

        @pl.when(same)
        def _():
            qr[slot] = qs[lax.div(tx, 2)]

        return carry

    lax.fori_loop(0, 16, send_heads, 0)
    keeps_one = (lax.rem(y, 4) == ty4) & (tc4 == c)
    own_copy = pltpu.make_async_copy(arr.at[me], dec_mine, own_sem.at[0])
    own_copy.start()
    pages(0)
    each(1 + PAGES[0], GROUP, 4, arrange)

    copies[1].wait()
    slot_page = lax.broadcasted_iota(jnp.int32, (GROUP, GROUP * 8), 0)
    slot_at = lax.broadcasted_iota(jnp.int32, (GROUP, GROUP * 8), 1)
    widen = jnp.where(lax.div(slot_at, 8) == slot_page, 1.0, 0.0).astype(BF16)
    token = lax.rem(lax.broadcasted_iota(jnp.int32, (8, GROUP * 8), 1), 8).astype(F32)
    lane = lax.broadcasted_iota(jnp.int32, (8, TILE), 1)
    seen, cosines, sines = [], [], []
    for e in range(2):
        length = len_ref[my_group * 2 + e].astype(F32)
        row = jnp.broadcast_to(tables[e], (8, GROUP)).astype(F32).astype(BF16)
        seen.append(dot_n(row, widen) * 8.0 + token < length)
        angle = jnp.broadcast_to(freq[...], (8, TILE)) * length
        sine = jnp.sin(angle)
        cosines.append(jnp.cos(angle))
        sines.append(jnp.where(lane < HEAD_DIM // 2, -sine, sine))


    @pl.when(keeps_one)
    def _():
        take(qr.at[pl.ds(0, 15)], rs.at[1])

    @pl.when(jnp.logical_not(keeps_one))
    def _():
        take(qr.at[pl.ds(0, 16)], rs.at[1])

    copies[9].wait()

    qf[...] = qr[...].astype(F32)

    rows8 = lax.broadcasted_iota(jnp.int32, (8, TILE), 0)
    rows16 = lax.broadcasted_iota(jnp.int32, (16, TILE), 0)
    scale = (D / HEADS) ** (-0.5)
    message = jnp.zeros((16, TILE), F32)
    row0 = lax.rem(my_group, 4) * 2
    for e in range(2):
        cos, sin = cosines[e], sines[e]

        def head(i):
            low = jnp.broadcast_to(qf[2 * i, pl.ds(row0 + e, 1), :], (8, TILE))
            high = jnp.broadcast_to(qf[2 * i + 1, pl.ds(row0 + e, 1), :], (8, TILE))
            return jnp.where(lane < HEAD_DIM // 2, low, high)

        def turned(u):
            return (u * cos + pltpu.roll(u, HEAD_DIM // 2, 1) * sin).astype(BF16).astype(F32)

        q = [turned(head(i)) for i in range(4)]
        k = [turned(head(4 + a)) for a in range(2)]
        v = [head(6 + a) for a in range(2)]
        zero = jnp.zeros((8, TILE), F32)
        left = jnp.where(rows8 == 0, q[0], jnp.where(rows8 == 1, q[1], zero))
        right = jnp.where(rows8 == 2, q[2], jnp.where(rows8 == 3, q[3], zero))
        own_raw = jnp.sum(left * k[0] + right * k[1], axis=1, keepdims=True) * scale
        own = jnp.exp(capped(own_raw))
        both = jnp.concatenate([left, right], axis=1).astype(BF16)
        raw = dot_t(both, cache[0, e]) * scale
        weights = jnp.where(seen[e], jnp.exp(capped(raw)), 0.0)
        den = jnp.sum(weights, axis=1, keepdims=True) + own
        num = dot_n(weights.astype(BF16), cache[1, e])
        own_b = own.astype(BF16).astype(F32)
        out_l = (num[:, :TILE] + own_b * v[0]) / den
        out_r = (num[:, TILE:] + own_b * v[1]) / den
        rows = [out_l[0:1], out_l[1:2], out_r[2:3], out_r[3:4], k[0][0:1], k[1][0:1], v[0][0:1], v[1][0:1]]
        for j, row in enumerate(rows):
            message = jnp.where(rows16 == e * 8 + j, jnp.broadcast_to(row, (16, TILE)), message)
    att_buf[c, x2, xp, y2, yp] = message.astype(BF16)

    first_leg(att_buf, 2)
    pages(1)
    second_leg(att_buf, 2)
    pages(2)
    last_leg(att_buf, 2, 3)

    want = lax.broadcasted_iota(jnp.int32, (128, 256), 0)
    have = lax.broadcasted_iota(jnp.int32, (128, 256), 1)
    target = 8 * lax.rem(want, 32) + lax.div(want, 32)
    pick_q = jnp.where(have == target, 1.0, 0.0).astype(BF16)
    pick_kv = jnp.where(have == target + 4, 1.0, 0.0).astype(BF16)

    def by_slot(k):
        blocks = []
        for g in range(16):
            ay = (g % 2) * 4 + k // 2
            blocks.append(att_buf[k % 2, g // 4, (g // 2) % 2, ay // 2, ay % 2])
        return jnp.concatenate(blocks, axis=0)

    for k in range(PREFILL_TP):
        picked = dot_n(pick_q, by_slot(k)).astype(BF16)
        for h in range(4):
            att[:, pl.ds((4 * k + h) * TILE, TILE)] = picked[32 * h : 32 * h + 32]
    copies[6].wait()
    mixed_part = dot_t(att[...], wo[...]).astype(BF16)
    shift = lax.rem(me * COLS, TILE)
    src_col = lax.broadcasted_iota(jnp.int32, (COLS, TILE), 0)
    dst_col = lax.broadcasted_iota(jnp.int32, (COLS, TILE), 1)
    put0 = jnp.where(dst_col == lax.rem(src_col + shift, TILE), 1.0, 0.0).astype(BF16)
    put1 = jnp.where(dst_col == lax.rem(src_col + shift + 64, TILE), 1.0, 0.0).astype(BF16)
    mix_buf[c, x2, xp, y2, yp] = (dot_n(mixed_part[:16], put0) + dot_n(mixed_part[16:], put1)).astype(BF16)

    first_leg(mix_buf, 5)
    pages(4)
    request = lax.broadcasted_iota(jnp.int32, fresh_ref.shape, 0)
    place = me * 8 + lax.broadcasted_iota(jnp.int32, fresh_ref.shape, 1)
    position = jnp.zeros(fresh_ref.shape, jnp.int32)
    for r in range(fresh_ref.shape[0]):
        position = jnp.where(request == r, len_ref[r], position)
    fresh_ref[...] = jnp.where(position == place, 1, 0)
    for k in range(PREFILL_TP):
        picked = dot_n(pick_kv, by_slot(k)).astype(BF16)
        for a in range(2):
            nk_ref[:, pl.ds((2 * k + a) * TILE, TILE)] = picked[32 * a : 32 * a + 32]
            nv_ref[:, pl.ds((2 * k + a) * TILE, TILE)] = picked[64 + 32 * a : 96 + 32 * a]
    second_leg(mix_buf, 5)
    pages(5)
    last_leg(mix_buf, 5, 6)

    lane16 = lax.broadcasted_iota(jnp.int32, (16, TILE), 1)

    def join(p, carry):
        straight, turned = [], []
        for i in range(32):
            piece = mix_buf[i % 2, p, i // 16, (i % 16) // 4, (i // 2) % 2].astype(F32)
            straight.append(piece)
            turned.append(pltpu.roll(piece, 64, 1))
        for t in range(9):
            top = bottom = None
            for i in range(32):
                lo, hi = COLS * i - TILE * t, COLS * i + COLS - TILE * t
                if hi <= 0 or lo >= TILE:
                    continue
                if top is None:
                    top, bottom = straight[i], turned[i]
                else:
                    later = lane16 >= lo
                    top = jnp.where(later, straight[i], top)
                    bottom = jnp.where(later, turned[i], bottom)
            column = pl.multiple_of((p * 9 + t) * TILE, TILE)
            mix[0:16, pl.ds(column, TILE)] = top
            mix[16:32, pl.ds(column, TILE)] = bottom
        return carry

    lax.fori_loop(0, 4, join, 0)
    stream[...] = hid[...] + rms_scale(mix[...], gain[1:2, :])
    ffn_in = rms_scale(stream[...], gain[2:3, :]).astype(BF16)
    copies[7].wait()
    gate = dot_t(ffn_in, wg[0])
    up = dot_t(ffn_in, wg[1])
    cube = gate + 0.044715 * (gate * gate * gate)
    active = (0.5 * gate * (1.0 + jnp.tanh(0.7978845608028654 * cube)) * up).astype(BF16)
    copies[8].wait()
    for n in range(4):
        columns = pl.ds(n * (D // 4), D // 4)
        piece = dot_n(active, wd[:, columns]).astype(BF16)
        br[0, :, columns] = piece[:16]
        br[1, :, columns] = piece[16:]

    send(br.at[1 - c], pr, 8, at(x, y, 1 - c))
    take(pr, rs.at[8])
    sb[...] = (br[c].astype(F32) + pr[...].astype(F32)).astype(BF16)

    def send_sums(j):
        owner = lax.div(j * 16, 9)
        tile = sb.at[:, pl.ds(pl.multiple_of(j * TILE, TILE), TILE)]

        @pl.when(owner != chip)
        def _():
            send(tile, rs_buf.at[chip], 9, at(lax.div(owner, NY), lax.rem(owner, NY), c))

        @pl.when(owner == chip)
        def _():
            rs_buf[chip] = tile[...]

    each(0, TILES, 6, send_sums)
    pages(7)
    my_tile = lax.div(chip * 9 + 15, 16)
    owns = lax.div(my_tile * 16, 9) == chip
    chip_cols = NC * COLS
    last_reader = lax.div(my_tile * TILE + TILE - 1, chip_cols)
    low = lax.div(chip * chip_cols, TILE)
    high = lax.div(chip * chip_cols + chip_cols - 1, TILE)
    low_tile = jnp.minimum(low, TILES - 2)
    needs_low = lax.div(low * 16, 9) != chip
    needs_high = (high != low) & (lax.div(high * 16, 9) != chip)

    @pl.when(owns)
    def _():
        take(rs_buf.at[pl.ds(0, CHIPS - 1)], rs.at[9])
        total = jnp.zeros((16, TILE), F32)

        def add(i, acc):
            for n in range(8):
                acc = acc + rs_buf[i * 8 + n].astype(F32)
            return acc

        total = lax.fori_loop(0, 8, add, total)
        fin[c, my_tile] = total.astype(BF16)
        squares = jnp.sum(total * total, axis=1, keepdims=True)
        sqs[c, my_tile] = jnp.sum(jnp.where(rows16 == lane16, squares, 0.0), axis=0, keepdims=True)
        for ahead in (1, 2):

            @pl.when(chip + ahead <= last_reader)
            def _():
                reader = chip + ahead
                send(fin.at[c, my_tile], fin.at[c, my_tile], 12, at(lax.div(reader, NY), lax.rem(reader, NY), c))

        def tell(i):
            tx, ty = other_chip(i)
            send(sqs.at[c, my_tile], sqs.at[c, my_tile], 10, at(tx, ty, c))

        each(0, CHIPS - 1, 9, tell)

    pages(8)

    @pl.when(owns)
    def _():
        take(sqs.at[0, pl.ds(0, TILES - 1)], rs.at[10])

    @pl.when(jnp.logical_not(owns))
    def _():
        take(sqs.at[0, pl.ds(0, TILES)], rs.at[10])

    @pl.when(needs_low & needs_high)
    def _():
        take(fin.at[0, pl.ds(0, 2)], rs.at[12])

    @pl.when(needs_low != needs_high)
    def _():
        take(fin.at[0, pl.ds(0, 1)], rs.at[12])

    swap(sqs, 11)
    send(fin.at[c, pl.ds(low_tile, 2)], fin.at[c, pl.ds(low_tile, 2)], 13, at(x, y, 1 - c))
    take(sqs.at[0], rs.at[11])
    take(fin.at[0, pl.ds(0, 2)], rs.at[13])

    first = lax.div(me * COLS, TILE)
    second = jnp.minimum(first + 1, TILES - 1)
    for half in range(2):

        squares = jnp.zeros((1, TILE), F32)
        for t in range(TILES):
            squares = squares + sqs[half, t]
        by_row = jnp.where(rows16 == lane16, jnp.broadcast_to(squares, (16, TILE)), 0.0)
        factor = lax.rsqrt(jnp.sum(by_row, axis=1, keepdims=True) / D + EPSILON)

        def block(t):
            columns = pl.ds(pl.multiple_of(t * TILE, TILE), TILE)
            branch = fin[half, t].astype(F32)
            value = stream[16 * half : 16 * half + 16, columns] + branch * factor * (1.0 + gain[3:4, columns])
            return pltpu.roll(value, lax.rem(TILE - shift, TILE), 1)

        value = jnp.where(lane16 < TILE - shift, block(first), block(second))
        res_ref[16 * half : 16 * half + 16, :] = value[:, :COLS]

    own_copy.wait()
    take(arr.at[pl.ds(0, GROUP - 1)], rs.at[0])
    take(arr.at[pl.ds(0, GROUP - 1)], ss.at[0])

    @pl.when(keeps_one)
    def _():
        take(qr.at[pl.ds(0, 15)], ss.at[1])

    @pl.when(jnp.logical_not(keeps_one))
    def _():
        take(qr.at[pl.ds(0, 16)], ss.at[1])

    gone(att_buf, 2)
    gone(mix_buf, 5)
    take(pr, ss.at[8])

    @pl.when(owns)
    def _():
        take(fin.at[0, pl.ds(0, TILES - 1)], ss.at[9])
        take(marks, ss.at[10])

        @pl.when(chip + 2 <= last_reader)
        def _():
            take(fin.at[0, pl.ds(0, 2)], ss.at[12])

        @pl.when((chip + 1 <= last_reader) & (chip + 2 > last_reader))
        def _():
            take(fin.at[0, pl.ds(0, 1)], ss.at[12])

    @pl.when(jnp.logical_not(owns))
    def _():
        take(fin.at[0, pl.ds(0, TILES)], ss.at[9])

    take(sqs.at[0], ss.at[11])
    take(fin.at[0, pl.ds(0, 2)], ss.at[13])


def on_device(
    hidden_in,
    prefill_cache,
    lengths,
    page_table,
    qkv_weight,
    out_weight,
    gate_up_weight,
    down_weight,
    norm_gains,
):
    batch = hidden_in.shape[0]
    page_width = prefill_cache.shape[5]
    exponent = np.arange(HEAD_DIM // 2, dtype=np.float32) * np.float32(-2.0 / HEAD_DIM)
    frequency = np.power(np.float32(10000.0), exponent).astype(np.float32)
    frequency = jnp.asarray(np.concatenate([frequency, frequency])[None, :])
    paged = prefill_cache.reshape(2, 2, GROUP, page_width, 2 * HEAD_DIM)
    cache = prefill_cache.reshape(2, 2, GROUP * page_width, 2 * HEAD_DIM)
    k_cols = KV_HEADS * HEAD_DIM
    vmem = pl.BlockSpec(memory_space=pltpu.VMEM)
    hbm = pl.BlockSpec(memory_space=pltpu.HBM)
    dma = pltpu.SemaphoreType.DMA
    res, new_key, new_value, fresh, decoded = pl.pallas_call(
        step_kernel,
        name="step",
        out_shape=(
            jax.ShapeDtypeStruct((batch, COLS), F32),
            jax.ShapeDtypeStruct((batch, k_cols), BF16),
            jax.ShapeDtypeStruct((batch, k_cols), BF16),
            jax.ShapeDtypeStruct((batch, page_width), jnp.int32),
            jax.ShapeDtypeStruct((1, 1, 2, batch, page_width, k_cols), BF16),
        ),
        in_specs=[pl.BlockSpec(memory_space=pltpu.SMEM)] + [hbm] * 10,
        out_specs=(vmem, vmem, vmem, vmem, pl.BlockSpec(memory_space=pl.ANY)),
        scratch_shapes=[
            pltpu.VMEM(page_table.shape, jnp.int32),
            pltpu.VMEM(frequency.shape, F32),
            pltpu.VMEM((16, GROUP), jnp.int32),
            pltpu.SMEM((16, GROUP), jnp.int32),
            pltpu.VMEM((batch, D), F32),
            pltpu.VMEM(paged.shape, BF16),
            pltpu.VMEM(cache.shape, BF16),
            pltpu.VMEM(qkv_weight.shape[1:], BF16),
            pltpu.VMEM(out_weight.shape[1:], BF16),
            pltpu.VMEM(gate_up_weight.shape[1:], BF16),
            pltpu.VMEM(down_weight.shape[1:], BF16),
            pltpu.VMEM(norm_gains.shape[1:], F32),
            pltpu.VMEM((GROUP, 2, 2, page_width, 2 * HEAD_DIM), BF16),
            pltpu.VMEM((4, 8, TILE), BF16),
            pltpu.VMEM((16, 8, TILE), BF16),
            pltpu.VMEM((16, 8, TILE), F32),
            pltpu.VMEM((NC, NX // 2, 2, NY // 2, 2, 16, TILE), BF16),
            pltpu.VMEM((batch, HEADS * HEAD_DIM), BF16),
            pltpu.VMEM((NC, NX // 2, 2, NY // 2, 2, 16, TILE), BF16),
            pltpu.VMEM((batch, D), F32),
            pltpu.VMEM((batch, D), F32),
            pltpu.VMEM((2, 16, D), BF16),
            pltpu.VMEM((16, D), BF16),
            pltpu.VMEM((16, D), BF16),
            pltpu.VMEM((CHIPS, 16, TILE), BF16),
            pltpu.VMEM((NC, TILES, 16, TILE), BF16),
            pltpu.VMEM((NC, TILES, 1, TILE), F32),
            pltpu.VMEM((CHIPS - 1, 1, TILE), F32),
            dma((10,)),
            dma((2,)),
            dma((14,)),
            dma((14,)),
        ],
        compiler_params=pltpu.CompilerParams(
            collective_id=0, has_side_effects=True, vmem_limit_bytes=48 * 2**20
        ),
    )(
        *[
            pltpu.with_memory_space_constraint(operand, pltpu.HBM)
            for operand in (
                lengths, page_table, frequency, hidden_in, paged, cache,
                qkv_weight, out_weight, gate_up_weight, down_weight, norm_gains,
            )
        ]
    )
    fresh = (fresh != 0)[None, None, None, :, :, None]
    new = jnp.stack([new_key, new_value], axis=0).reshape(1, 1, 2, batch, 1, k_cols)
    decode_cache = jnp.where(fresh, new, decoded)
    return (res, decode_cache)


def solution(mesh):
    torus = Mesh(mesh.devices.reshape(mesh.shape["grp"], NX, NY, NC), ("grp",) + TP)
    return jax.shard_map(
        on_device,
        mesh=torus,
        in_specs=(
            P("grp", None),
            P(TP, None, None, "grp", None, None, None),
            P("grp"),
            P("grp", None),
            P(None, TP, None),
            P(None, TP, None),
            P(None, None, TP, None),
            P(None, TP, None),
            P(),
        ),
        out_specs=(P("grp", TP), P(TP, None, None, "grp", None, None)),
        check_vma=False,
    )
```

```python
import jax
import jax.numpy as jnp
import numpy as np
from jax import lax
from jax.experimental import pallas as pl
from jax.experimental.pallas import tpu as pltpu
from jax.sharding import Mesh
from jax.sharding import PartitionSpec as P

D = 4608
HEADS = 32
KV_HEADS = 16
HEAD_DIM = 128
PREFILL_TP = 8
NX, NY, NC = 8, 8, 2
CHIPS = NX * NY
GROUP = CHIPS * NC
COLS = D // GROUP
TILE = 128
TILES = D // TILE
TP = ("tp_0", "tp_1", "tp_2")
MESH = pl.DeviceIdType.MESH
BF16 = jnp.bfloat16
F32 = jnp.float32

EPSILON = 1e-06
SOFTCAP = 50.0

PAGES = (24, 12, 18, 0, 12, 18, 0, 20, 23)


def capped(raw_scores):
    return SOFTCAP * jnp.tanh(raw_scores / SOFTCAP)


def rms_scale(vector, gain_row):
    meansq = jnp.mean(vector * vector, axis=-1, keepdims=True)
    return vector * lax.rsqrt(meansq + EPSILON) * (1.0 + gain_row)


def dot_t(left, right):
    return lax.dot_general(left, right, (((1,), (1,)), ((), ())), preferred_element_type=F32)


def dot_n(left, right):
    return jnp.dot(left, right, preferred_element_type=F32)


def step_kernel(
    len_ref, table_hbm, freq_hbm, hid_hbm, paged_hbm, cache_hbm, wq_hbm, wo_hbm, wg_hbm, wd_hbm, gain_hbm,
    res_ref, nk_ref, nv_ref, fresh_ref, dec_ref,
    table, freq, inv_v, inv, hid, paged, cache, wq, wo, wg, wd, gain, arr, qs, qr, qf, att_buf, att, mix_buf, mix, stream,
    br, pr, sb, rs_buf, fin, sqs, marks, in_sem, own_sem, ss, rs,
):
    grp = lax.axis_index("grp")
    x = lax.axis_index("tp_0")
    y = lax.axis_index("tp_1")
    c = lax.axis_index("tp_2")
    chip = x * NY + y
    me = chip * NC + c
    my_group = lax.div(me, PREFILL_TP)
    my_slot = lax.rem(me, PREFILL_TP)

    def at(tx, ty, tc):
        return (grp, tx, ty, tc)

    barrier = pltpu.get_barrier_semaphore()

    def peer(i):
        tx = lax.rem(x + lax.div(i, NY * NC), NX)
        ty = lax.rem(y + lax.rem(lax.div(i, NC), NY), NY)
        tc = lax.rem(c + lax.rem(i, NC), NC)
        return tx, ty, tc

    all_y = [lax.rem(y + n, NY) for n in (4, 3, 5, 2, 6, 1, 7, 0)]

    def greet(tx, ty, tc):
        pl.semaphore_signal(barrier, inc=1, device_id=at(tx, ty, tc), device_id_type=MESH)

    def greet_row(n, carry):
        tx = lax.rem(x + 1 + n, NX)
        for ty in all_y:
            greet(tx, ty, c)
            greet(tx, ty, 1 - c)
        return carry

    loads = [
        (table_hbm, table), (freq_hbm, freq), (hid_hbm, hid),
        (gain_hbm.at[0], gain), (wq_hbm.at[0], wq), (paged_hbm, paged),
        (wo_hbm.at[0], wo), (wg_hbm.at[0], wg), (wd_hbm.at[0], wd), (cache_hbm, cache),
    ]
    copies = [pltpu.make_async_copy(s, d, in_sem.at[n]) for n, (s, d) in enumerate(loads)]
    for copy in copies:
        copy.start()
    lax.fori_loop(0, NX - 1, greet_row, 0)
    for ty in all_y[:-1]:
        greet(x, ty, c)
        greet(x, ty, 1 - c)
    greet(x, y, 1 - c)

    def send(src, dst, phase, target):
        pltpu.make_async_remote_copy(
            src_ref=src, dst_ref=dst, send_sem=ss.at[phase], recv_sem=rs.at[phase],
            device_id=target, device_id_type=MESH,
        ).start()

    def take(ref, sem):
        pltpu.make_async_copy(ref, ref, sem).wait()

    def each(first, last, width, body):
        whole = (last - first) // width

        def several(n, carry):
            for k in range(width):
                body(first + n * width + k)
            return carry

        if whole:
            lax.fori_loop(0, whole, several, 0)
        for n in range(first + whole * width, last):
            body(n)

    dec_mine = dec_ref.at[0, 0, :, pl.ds(my_group * 2, 2), :, pl.ds(pl.multiple_of(my_slot * 256, 256), 256)]

    def page_peer(j):
        tx, ty, tc = peer(lax.rem(j * 53, GROUP))
        return (tx * NY + ty) * NC + tc, at(tx, ty, tc)

    def send_page(j):
        number, target = page_peer(j)
        send(arr.at[number], dec_mine, 0, target)

    def arrange(j):
        number, _ = page_peer(j)
        for e in range(2):
            page = jnp.maximum(jnp.minimum(inv[8 * e, number], GROUP - 1), 0)
            for kv in range(2):
                arr[number, kv, e] = paged[kv, e, page]

    def pages(n):
        first = 1 + sum(PAGES[:n])
        each(first, first + PAGES[n], 4, send_page)

    def other_chip(i):
        n = i + lax.div(i, 36)
        tx = lax.rem(x + 4 + lax.div(n, NY), NX)
        ty = lax.rem(y + 4 + lax.rem(n, NY), NY)
        return tx, ty

    x2, xp, y2, yp = lax.div(x, 2), lax.rem(x, 2), lax.div(y, 2), lax.rem(y, 2)
    even = 1 - lax.rem(x + y, 2)

    def mine(buf):
        return buf.at[c, x2, xp, y2, yp]

    def first_leg(buf, phase):
        for o in (4, 3, 5, 2, 6, 1, 7):
            target = at(lax.rem(x + even * o, NX), lax.rem(y + (1 - even) * o, NY), c)
            send(mine(buf), mine(buf), phase, target)

    def second_leg(buf, phase):
        take(rs_buf.at[pl.ds(0, 7)], rs.at[phase])
        row = buf.at[c, :, yp, y2, yp]
        column = buf.at[c, x2, xp, :, 1 - xp]
        for o in (4, 3, 5, 2, 6, 1, 7):
            send(row, row, phase + 1, at(x, lax.rem(y + o, NY), c))
            send(column, column, phase + 1, at(lax.rem(x + o, NX), y, c))

    def last_leg(buf, phase, portion):
        take(rs_buf.at[pl.ds(0, 56)], rs.at[phase + 1])
        swap(buf, phase + 2)
        pages(portion)
        take(buf.at[0], rs.at[phase + 2])

    def gone(buf, phase):
        take(rs_buf.at[pl.ds(0, 7)], ss.at[phase])
        take(rs_buf.at[pl.ds(0, 56)], ss.at[phase + 1])
        take(buf.at[0], ss.at[phase + 2])

    def swap(buf, phase):
        send(buf.at[c], buf.at[c], phase, at(x, y, 1 - c))

    copies[2].wait()
    copies[3].wait()
    normed = rms_scale(hid[...], gain[0:1, :]).astype(BF16)
    copies[4].wait()
    part = dot_t(normed, wq[...]).astype(BF16)
    part = jnp.concatenate([part, part], axis=1)
    for t in range(4):
        qs[t] = part[8 * t : 8 * t + 8]

    copies[0].wait()
    block = lax.broadcasted_iota(jnp.int32, (GROUP, GROUP), 0)
    index = lax.broadcasted_iota(jnp.int32, (8, GROUP), 1).astype(F32).astype(BF16)
    tables = []
    for e in range(2):
        row = table[pl.ds(my_group * 2 + e, 1), :]
        tables.append(row)
        hits = jnp.where(jnp.broadcast_to(row, (GROUP, GROUP)) == block, 1.0, 0.0).astype(BF16)
        inv_v[8 * e : 8 * e + 8, :] = dot_t(index, hits).astype(jnp.int32)
    to_scalars = pltpu.make_async_copy(inv_v, inv, own_sem.at[1])
    to_scalars.start()

    copies[5].wait()
    to_scalars.wait()

    each(0, 1 + PAGES[0], 4, arrange)
    fin[...] = jnp.zeros(fin.shape, BF16)
    pl.semaphore_wait(barrier, GROUP - 1)

    is_kv = lax.div(x, 4)
    xx = lax.rem(x, 2)
    ty4 = (1 - is_kv) * x + is_kv * (xx * 2 + lax.div(y, 4))
    tc4 = (1 - is_kv) * lax.div(y, 4) + is_kv * lax.rem(lax.div(y, 2), 2)
    slot = (1 - is_kv) * (lax.rem(y, 4) * 2 + c) + is_kv * (
        8 + lax.div(lax.rem(x, 4), 2) * 4 + lax.rem(y, 2) * 2 + c
    )

    def send_heads(i, carry):
        tx = lax.rem(x + lax.div(i, 2), NX)
        ty = ty4 + 4 * lax.rem(i, 2)
        same = (tx == x) & (ty == y) & (tc4 == c)

        @pl.when(jnp.logical_not(same))
        def _():
            send(qs.at[lax.div(tx, 2)], qr.at[slot], 1, at(tx, ty, tc4))

        @pl.when(same)
        def _():
            qr[slot] = qs[lax.div(tx, 2)]

        return carry

    lax.fori_loop(0, 16, send_heads, 0)
    keeps_one = (lax.rem(y, 4) == ty4) & (tc4 == c)
    own_copy = pltpu.make_async_copy(arr.at[me], dec_mine, own_sem.at[0])
    own_copy.start()
    pages(0)
    each(1 + PAGES[0], GROUP, 4, arrange)

    copies[1].wait()
    slot_page = lax.broadcasted_iota(jnp.int32, (GROUP, GROUP * 8), 0)
    slot_at = lax.broadcasted_iota(jnp.int32, (GROUP, GROUP * 8), 1)
    widen = jnp.where(lax.div(slot_at, 8) == slot_page, 1.0, 0.0).astype(BF16)
    token = lax.rem(lax.broadcasted_iota(jnp.int32, (8, GROUP * 8), 1), 8).astype(F32)
    lane = lax.broadcasted_iota(jnp.int32, (8, TILE), 1)
    seen, cosines, sines = [], [], []
    for e in range(2):
        length = len_ref[my_group * 2 + e].astype(F32)
        row = jnp.broadcast_to(tables[e], (8, GROUP)).astype(F32).astype(BF16)
        seen.append(dot_n(row, widen) * 8.0 + token < length)
        angle = jnp.broadcast_to(freq[...], (8, TILE)) * length
        sine = jnp.sin(angle)
        cosines.append(jnp.cos(angle))
        sines.append(jnp.where(lane < HEAD_DIM // 2, -sine, sine))


    @pl.when(keeps_one)
    def _():
        take(qr.at[pl.ds(0, 15)], rs.at[1])

    @pl.when(jnp.logical_not(keeps_one))
    def _():
        take(qr.at[pl.ds(0, 16)], rs.at[1])

    copies[9].wait()

    qf[...] = qr[...].astype(F32)

    rows8 = lax.broadcasted_iota(jnp.int32, (8, TILE), 0)
    rows16 = lax.broadcasted_iota(jnp.int32, (16, TILE), 0)
    scale = (D / HEADS) ** (-0.5)
    message = jnp.zeros((16, TILE), F32)
    row0 = lax.rem(my_group, 4) * 2
    for e in range(2):
        cos, sin = cosines[e], sines[e]

        def head(i):
            low = jnp.broadcast_to(qf[2 * i, pl.ds(row0 + e, 1), :], (8, TILE))
            high = jnp.broadcast_to(qf[2 * i + 1, pl.ds(row0 + e, 1), :], (8, TILE))
            return jnp.where(lane < HEAD_DIM // 2, low, high)

        def turned(u):
            return (u * cos + pltpu.roll(u, HEAD_DIM // 2, 1) * sin).astype(BF16).astype(F32)

        q = [turned(head(i)) for i in range(4)]
        k = [turned(head(4 + a)) for a in range(2)]
        v = [head(6 + a) for a in range(2)]
        zero = jnp.zeros((8, TILE), F32)
        left = jnp.where(rows8 == 0, q[0], jnp.where(rows8 == 1, q[1], zero))
        right = jnp.where(rows8 == 2, q[2], jnp.where(rows8 == 3, q[3], zero))
        own_raw = jnp.sum(left * k[0] + right * k[1], axis=1, keepdims=True) * scale
        own = jnp.exp(capped(own_raw))
        both = jnp.concatenate([left, right], axis=1).astype(BF16)
        raw = dot_t(both, cache[0, e]) * scale
        weights = jnp.where(seen[e], jnp.exp(capped(raw)), 0.0)
        den = jnp.sum(weights, axis=1, keepdims=True) + own
        num = dot_n(weights.astype(BF16), cache[1, e])
        own_b = own.astype(BF16).astype(F32)
        out_l = (num[:, :TILE] + own_b * v[0]) / den
        out_r = (num[:, TILE:] + own_b * v[1]) / den
        rows = [out_l[0:1], out_l[1:2], out_r[2:3], out_r[3:4], k[0][0:1], k[1][0:1], v[0][0:1], v[1][0:1]]
        for j, row in enumerate(rows):
            message = jnp.where(rows16 == e * 8 + j, jnp.broadcast_to(row, (16, TILE)), message)
    att_buf[c, x2, xp, y2, yp] = message.astype(BF16)

    first_leg(att_buf, 2)
    pages(1)
    second_leg(att_buf, 2)
    pages(2)
    last_leg(att_buf, 2, 3)

    want = lax.broadcasted_iota(jnp.int32, (128, 256), 0)
    have = lax.broadcasted_iota(jnp.int32, (128, 256), 1)
    target = 8 * lax.rem(want, 32) + lax.div(want, 32)
    pick_q = jnp.where(have == target, 1.0, 0.0).astype(BF16)
    pick_kv = jnp.where(have == target + 4, 1.0, 0.0).astype(BF16)

    def by_slot(k):
        blocks = []
        for g in range(16):
            ay = (g % 2) * 4 + k // 2
            blocks.append(att_buf[k % 2, g // 4, (g // 2) % 2, ay // 2, ay % 2])
        return jnp.concatenate(blocks, axis=0)

    for k in range(PREFILL_TP):
        picked = dot_n(pick_q, by_slot(k)).astype(BF16)
        for h in range(4):
            att[:, pl.ds((4 * k + h) * TILE, TILE)] = picked[32 * h : 32 * h + 32]
    copies[6].wait()
    mixed_part = dot_t(att[...], wo[...]).astype(BF16)
    shift = lax.rem(me * COLS, TILE)
    src_col = lax.broadcasted_iota(jnp.int32, (COLS, TILE), 0)
    dst_col = lax.broadcasted_iota(jnp.int32, (COLS, TILE), 1)
    put0 = jnp.where(dst_col == lax.rem(src_col + shift, TILE), 1.0, 0.0).astype(BF16)
    put1 = jnp.where(dst_col == lax.rem(src_col + shift + 64, TILE), 1.0, 0.0).astype(BF16)
    mix_buf[c, x2, xp, y2, yp] = (dot_n(mixed_part[:16], put0) + dot_n(mixed_part[16:], put1)).astype(BF16)

    first_leg(mix_buf, 5)
    pages(4)
    request = lax.broadcasted_iota(jnp.int32, fresh_ref.shape, 0)
    place = me * 8 + lax.broadcasted_iota(jnp.int32, fresh_ref.shape, 1)
    position = jnp.zeros(fresh_ref.shape, jnp.int32)
    for r in range(fresh_ref.shape[0]):
        position = jnp.where(request == r, len_ref[r], position)
    fresh_ref[...] = jnp.where(position == place, 1, 0)
    for k in range(PREFILL_TP):
        picked = dot_n(pick_kv, by_slot(k)).astype(BF16)
        for a in range(2):
            nk_ref[:, pl.ds((2 * k + a) * TILE, TILE)] = picked[32 * a : 32 * a + 32]
            nv_ref[:, pl.ds((2 * k + a) * TILE, TILE)] = picked[64 + 32 * a : 96 + 32 * a]
    second_leg(mix_buf, 5)
    pages(5)
    last_leg(mix_buf, 5, 6)

    lane16 = lax.broadcasted_iota(jnp.int32, (16, TILE), 1)

    def join(p, carry):
        straight, turned = [], []
        for i in range(32):
            piece = mix_buf[i % 2, p, i // 16, (i % 16) // 4, (i // 2) % 2].astype(F32)
            straight.append(piece)
            turned.append(pltpu.roll(piece, 64, 1))
        for t in range(9):
            top = bottom = None
            for i in range(32):
                lo, hi = COLS * i - TILE * t, COLS * i + COLS - TILE * t
                if hi <= 0 or lo >= TILE:
                    continue
                if top is None:
                    top, bottom = straight[i], turned[i]
                else:
                    later = lane16 >= lo
                    top = jnp.where(later, straight[i], top)
                    bottom = jnp.where(later, turned[i], bottom)
            column = pl.multiple_of((p * 9 + t) * TILE, TILE)
            mix[0:16, pl.ds(column, TILE)] = top
            mix[16:32, pl.ds(column, TILE)] = bottom
        return carry

    lax.fori_loop(0, 4, join, 0)
    stream[...] = hid[...] + rms_scale(mix[...], gain[1:2, :])
    ffn_in = rms_scale(stream[...], gain[2:3, :]).astype(BF16)
    copies[7].wait()
    gate = dot_t(ffn_in, wg[0])
    up = dot_t(ffn_in, wg[1])
    cube = gate + 0.044715 * (gate * gate * gate)
    active = (0.5 * gate * (1.0 + jnp.tanh(0.7978845608028654 * cube)) * up).astype(BF16)
    copies[8].wait()
    for n in range(4):
        columns = pl.ds(n * (D // 4), D // 4)
        piece = dot_n(active, wd[:, columns]).astype(BF16)
        br[0, :, columns] = piece[:16]
        br[1, :, columns] = piece[16:]

    send(br.at[1 - c], pr, 8, at(x, y, 1 - c))
    take(pr, rs.at[8])
    sb[...] = (br[c].astype(F32) + pr[...].astype(F32)).astype(BF16)

    def send_sums(j):
        owner = lax.div(j * 16, 9)
        tile = sb.at[:, pl.ds(pl.multiple_of(j * TILE, TILE), TILE)]

        @pl.when(owner != chip)
        def _():
            send(tile, rs_buf.at[chip], 9, at(lax.div(owner, NY), lax.rem(owner, NY), c))

        @pl.when(owner == chip)
        def _():
            rs_buf[chip] = tile[...]

    each(0, TILES, 6, send_sums)
    pages(7)
    my_tile = lax.div(chip * 9 + 15, 16)
    owns = lax.div(my_tile * 16, 9) == chip
    chip_cols = NC * COLS
    last_reader = lax.div(my_tile * TILE + TILE - 1, chip_cols)
    low = lax.div(chip * chip_cols, TILE)
    high = lax.div(chip * chip_cols + chip_cols - 1, TILE)
    low_tile = jnp.minimum(low, TILES - 2)
    needs_low = lax.div(low * 16, 9) != chip
    needs_high = (high != low) & (lax.div(high * 16, 9) != chip)

    @pl.when(owns)
    def _():
        take(rs_buf.at[pl.ds(0, CHIPS - 1)], rs.at[9])
        total = jnp.zeros((16, TILE), F32)

        def add(i, acc):
            for n in range(8):
                acc = acc + rs_buf[i * 8 + n].astype(F32)
            return acc

        total = lax.fori_loop(0, 8, add, total)
        fin[c, my_tile] = total.astype(BF16)
        squares = jnp.sum(total * total, axis=1, keepdims=True)
        sqs[c, my_tile] = jnp.sum(jnp.where(rows16 == lane16, squares, 0.0), axis=0, keepdims=True)
        for ahead in (1, 2):

            @pl.when(chip + ahead <= last_reader)
            def _():
                reader = chip + ahead
                send(fin.at[c, my_tile], fin.at[c, my_tile], 12, at(lax.div(reader, NY), lax.rem(reader, NY), c))

        def tell(i):
            tx, ty = other_chip(i)
            send(sqs.at[c, my_tile], sqs.at[c, my_tile], 10, at(tx, ty, c))

        each(0, CHIPS - 1, 9, tell)

    pages(8)

    @pl.when(owns)
    def _():
        take(sqs.at[0, pl.ds(0, TILES - 1)], rs.at[10])

    @pl.when(jnp.logical_not(owns))
    def _():
        take(sqs.at[0, pl.ds(0, TILES)], rs.at[10])

    @pl.when(needs_low & needs_high)
    def _():
        take(fin.at[0, pl.ds(0, 2)], rs.at[12])

    @pl.when(needs_low != needs_high)
    def _():
        take(fin.at[0, pl.ds(0, 1)], rs.at[12])

    swap(sqs, 11)
    send(fin.at[c, pl.ds(low_tile, 2)], fin.at[c, pl.ds(low_tile, 2)], 13, at(x, y, 1 - c))
    take(sqs.at[0], rs.at[11])
    take(fin.at[0, pl.ds(0, 2)], rs.at[13])

    first = lax.div(me * COLS, TILE)
    second = jnp.minimum(first + 1, TILES - 1)
    for half in range(2):

        squares = jnp.zeros((1, TILE), F32)
        for t in range(TILES):
            squares = squares + sqs[half, t]
        by_row = jnp.where(rows16 == lane16, jnp.broadcast_to(squares, (16, TILE)), 0.0)
        factor = lax.rsqrt(jnp.sum(by_row, axis=1, keepdims=True) / D + EPSILON)

        def block(t):
            columns = pl.ds(pl.multiple_of(t * TILE, TILE), TILE)
            branch = fin[half, t].astype(F32)
            value = stream[16 * half : 16 * half + 16, columns] + branch * factor * (1.0 + gain[3:4, columns])
            return pltpu.roll(value, lax.rem(TILE - shift, TILE), 1)

        value = jnp.where(lane16 < TILE - shift, block(first), block(second))
        res_ref[16 * half : 16 * half + 16, :] = value[:, :COLS]

    own_copy.wait()
    take(arr.at[pl.ds(0, GROUP - 1)], rs.at[0])
    take(arr.at[pl.ds(0, GROUP - 1)], ss.at[0])

    @pl.when(keeps_one)
    def _():
        take(qr.at[pl.ds(0, 15)], ss.at[1])

    @pl.when(jnp.logical_not(keeps_one))
    def _():
        take(qr.at[pl.ds(0, 16)], ss.at[1])

    gone(att_buf, 2)
    gone(mix_buf, 5)
    take(pr, ss.at[8])

    @pl.when(owns)
    def _():
        take(fin.at[0, pl.ds(0, TILES - 1)], ss.at[9])
        take(marks, ss.at[10])

        @pl.when(chip + 2 <= last_reader)
        def _():
            take(fin.at[0, pl.ds(0, 2)], ss.at[12])

        @pl.when((chip + 1 <= last_reader) & (chip + 2 > last_reader))
        def _():
            take(fin.at[0, pl.ds(0, 1)], ss.at[12])

    @pl.when(jnp.logical_not(owns))
    def _():
        take(fin.at[0, pl.ds(0, TILES)], ss.at[9])

    take(sqs.at[0], ss.at[11])
    take(fin.at[0, pl.ds(0, 2)], ss.at[13])


def on_device(
    hidden_in,
    prefill_cache,
    lengths,
    page_table,
    qkv_weight,
    out_weight,
    gate_up_weight,
    down_weight,
    norm_gains,
):
    batch = hidden_in.shape[0]
    page_width = prefill_cache.shape[5]
    exponent = np.arange(HEAD_DIM // 2, dtype=np.float32) * np.float32(-2.0 / HEAD_DIM)
    frequency = np.power(np.float32(10000.0), exponent).astype(np.float32)
    frequency = jnp.asarray(np.concatenate([frequency, frequency])[None, :])
    paged = prefill_cache.reshape(2, 2, GROUP, page_width, 2 * HEAD_DIM)
    cache = prefill_cache.reshape(2, 2, GROUP * page_width, 2 * HEAD_DIM)
    k_cols = KV_HEADS * HEAD_DIM
    vmem = pl.BlockSpec(memory_space=pltpu.VMEM)
    hbm = pl.BlockSpec(memory_space=pltpu.HBM)
    dma = pltpu.SemaphoreType.DMA
    res, new_key, new_value, fresh, decoded = pl.pallas_call(
        step_kernel,
        name="step",
        out_shape=(
            jax.ShapeDtypeStruct((batch, COLS), F32),
            jax.ShapeDtypeStruct((batch, k_cols), BF16),
            jax.ShapeDtypeStruct((batch, k_cols), BF16),
            jax.ShapeDtypeStruct((batch, page_width), jnp.int32),
            jax.ShapeDtypeStruct((1, 1, 2, batch, page_width, k_cols), BF16),
        ),
        in_specs=[pl.BlockSpec(memory_space=pltpu.SMEM)] + [hbm] * 10,
        out_specs=(vmem, vmem, vmem, vmem, pl.BlockSpec(memory_space=pl.ANY)),
        scratch_shapes=[
            pltpu.VMEM(page_table.shape, jnp.int32),
            pltpu.VMEM(frequency.shape, F32),
            pltpu.VMEM((16, GROUP), jnp.int32),
            pltpu.SMEM((16, GROUP), jnp.int32),
            pltpu.VMEM((batch, D), F32),
            pltpu.VMEM(paged.shape, BF16),
            pltpu.VMEM(cache.shape, BF16),
            pltpu.VMEM(qkv_weight.shape[1:], BF16),
            pltpu.VMEM(out_weight.shape[1:], BF16),
            pltpu.VMEM(gate_up_weight.shape[1:], BF16),
            pltpu.VMEM(down_weight.shape[1:], BF16),
            pltpu.VMEM(norm_gains.shape[1:], F32),
            pltpu.VMEM((GROUP, 2, 2, page_width, 2 * HEAD_DIM), BF16),
            pltpu.VMEM((4, 8, TILE), BF16),
            pltpu.VMEM((16, 8, TILE), BF16),
            pltpu.VMEM((16, 8, TILE), F32),
            pltpu.VMEM((NC, NX // 2, 2, NY // 2, 2, 16, TILE), BF16),
            pltpu.VMEM((batch, HEADS * HEAD_DIM), BF16),
            pltpu.VMEM((NC, NX // 2, 2, NY // 2, 2, 16, TILE), BF16),
            pltpu.VMEM((batch, D), F32),
            pltpu.VMEM((batch, D), F32),
            pltpu.VMEM((2, 16, D), BF16),
            pltpu.VMEM((16, D), BF16),
            pltpu.VMEM((16, D), BF16),
            pltpu.VMEM((CHIPS, 16, TILE), BF16),
            pltpu.VMEM((NC, TILES, 16, TILE), BF16),
            pltpu.VMEM((NC, TILES, 1, TILE), F32),
            pltpu.VMEM((CHIPS - 1, 1, TILE), F32),
            dma((10,)),
            dma((2,)),
            dma((14,)),
            dma((14,)),
        ],
        compiler_params=pltpu.CompilerParams(
            collective_id=0, has_side_effects=True, vmem_limit_bytes=48 * 2**20
        ),
    )(
        *[
            pltpu.with_memory_space_constraint(operand, pltpu.HBM)
            for operand in (
                lengths, page_table, frequency, hidden_in, paged, cache,
                qkv_weight, out_weight, gate_up_weight, down_weight, norm_gains,
            )
        ]
    )
    fresh = (fresh != 0)[None, None, None, :, :, None]
    new = jnp.stack([new_key, new_value], axis=0).reshape(1, 1, 2, batch, 1, k_cols)
    decode_cache = jnp.where(fresh, new, decoded)
    return (res, decode_cache)


def solution(mesh):
    torus = Mesh(mesh.devices.reshape(mesh.shape["grp"], NX, NY, NC), ("grp",) + TP)
    return jax.shard_map(
        on_device,
        mesh=torus,
        in_specs=(
            P("grp", None),
            P(TP, None, None, "grp", None, None, None),
            P("grp"),
            P("grp", None),
            P(None, TP, None),
            P(None, TP, None),
            P(None, None, TP, None),
            P(None, TP, None),
            P(),
        ),
        out_specs=(P("grp", TP), P(TP, None, None, "grp", None, None)),
        check_vma=False,
    )
```
